256 devices in a mesh: grp: 4 (over x), gx: 16 (over y, z_lo, core), gy: 4 (over z_hi).
Axes of the slice: x: 4, y: 4, z: 8 (z_hi: 4, z_lo: 2; z = z_hi * 2 + z_lo), core: 2. Of those that a mesh axis runs over, the one named last changes fastest.
Arguments:
- pressure_start: float32 [128, 32, 512], P('gx', 'gy', 'grp'), may hold values from -6 to 6
- saturation: float32 [128, 32, 512], P('gx', 'gy', 'grp'), may hold values from 0.1 to 0.9
- permeability: float32 [128, 32, 512], P('gx', 'gy', 'grp'), may hold values from 0.1 to 10
- rock_type: int32 [128, 32, 512], P('gx', 'gy', 'grp'), may hold values from 0 to 3
- rock_table: float32 [5, 4], replicated, may hold values from 0.5 to 3
- well_cells: int32 [64], replicated, may hold values from 0 to 2097151
- well_rates: float32 [64], replicated, may hold values from -12 to 12
- owner_map: int32 [16, 4, 4, 64, 1], P('gx', 'gy', 'grp'), may hold values from 0 to 15; in each aligned block of 64 rows (0 to 63, 64 to 127, ..., all dimensions but the last counted through in order) at most 8 rows name the same one
- stiffness: bfloat16 [16, 4, 4, 16, 8, 24, 24], P('gx', 'gy', 'grp'), may hold values from -0.008 to 0.2, as said below
- anchored: int32 [128, 32, 512], P('gx', 'gy', 'grp'), may hold values 0 or 1
Outputs:
- pressure: float32 [128, 32, 512], P('gx', 'gy', 'grp')
- vol_strain: float32 [128, 32, 512], P('gx', 'gy', 'grp')
The draws below stay inside these ranges and needn't reach their ends.
Inputs may be any that keep to these rules, and one draw needn't show every extreme that they name: `owner_map`: of the 64 bricks of one device, at most 8 have the same owner. `stiffness`: the diagonal entries of every block lie between 0.1 and 0.2.
All inputs are finite; a program needn't handle non-finite values. No bound on the sum of `anchored` on one device may be relied on, other than what follows from the above.
Results may differ from the reference program's by a relative error of at most 0.0013.
Values may be sent and summed in bfloat16 or wider, within the bound.
No kernel may reach another device: no remote copies, remote signals or barrier semaphores. Data moves between devices by JAX's collectives and lax.ppermute only.
A program may use at most 64 MiB of HBM per device.

```python
import math
import jax
import jax.numpy as jnp
import numpy as np
from jax import lax

CX = 8
CY = 8
CZ = 128
ITERS = 2
FLOW_PASSES = 4
MECH_PASSES = 3
ROCKS = 4
WELLS = 64
SLABS_X = 16
SLABS_Y = 4
LAYERS_Z = 4
BRICKS = 64
CAP = 8
NX = 128
NY = 32
NZ = 512
N_GRP = 4
N_GX = 16
N_GY = 4


def draw_stiffness(key, part):
    block_shape = (SLABS_X, SLABS_Y, LAYERS_Z, SLABS_X, CAP)
    first_key, second_key = jax.random.split(jax.random.fold_in(key, 7))
    diag_part = jax.random.uniform(first_key, block_shape, jnp.float32, 0.101, 0.195)
    off_part = jax.random.uniform(second_key, block_shape + (24, 24), jnp.float32, -0.0079, 0.0079)
    identity = jnp.eye(24, dtype=jnp.float32)
    blocks = off_part * (1.0 - identity) + diag_part[..., None, None] * identity
    return blocks.astype(jnp.bfloat16)


def set_ends(values, key, least, top_value):
    index_at = [jax.random.randint(jax.random.fold_in(key, axis), (), 0, length) for axis, length in enumerate(values.shape)]
    longest = values.shape.index(max(values.shape))
    neighbour = index_at[:longest] + [(index_at[longest] + 1) % values.shape[longest]] + index_at[longest + 1:]
    return values.at[tuple(index_at)].set(least).at[tuple(neighbour)].set(top_value)


def levels(key, dims, shards, least, largest):
    level = 1.0
    for axis_at, shards_of in shards:
        draws = jax.random.uniform(jax.random.fold_in(jax.random.fold_in(key, 6), axis_at), (shards_of,), jnp.float32, least / len(shards), largest / len(shards))
        level = level * jnp.repeat(jnp.exp(draws), dims[axis_at] // shards_of).reshape((-1,) + (1,) * (len(dims) - 1 - axis_at))
    return level


def assign_block(stream_key, own, number, rows, amount, top, most, lean):
    order = jax.random.permutation(stream_key, amount)
    crowded, usual = portions_of(amount, rows * top, most, lean, True), portions_of(amount, rows * top, most, lean, False)
    places = jnp.arange(amount)

    def named(lengths, turn):
        used = int((lengths > 0).sum())
        fixed = max(1, used // 4)
        shifted = fixed + (places - fixed + turn * (used - fixed)) % max(1, amount - fixed)
        return jnp.zeros((amount,), jnp.int32).at[order[jnp.where(places < fixed, places, shifted)]].set(jnp.asarray(lengths, jnp.int32))

    lengths = jnp.where(number % 4 == 0, named(crowded, number // 4), named(usual, number - number // 4 - 1))
    mixed = jax.random.permutation(jax.random.fold_in(own, 3), amount)
    source_of, receiver = mixed[0:amount // 2 * 2:2], mixed[1:amount // 2 * 2:2]
    slack = jnp.minimum(lengths[source_of] - 1, most - lengths[receiver]) // 2
    slack = jnp.where((source_of == order[0]) | (receiver == order[0]) | (lengths[receiver] == 0), 0, jnp.maximum(slack, 0))
    shifted = jax.random.randint(jax.random.fold_in(own, 4), (amount // 2,), 0, 1 << 20) % (slack + 1)
    lengths = lengths.at[source_of].add(-shifted).at[receiver].add(shifted)
    labels = jnp.searchsorted(jnp.cumsum(lengths), jnp.arange(rows * top), side="right").astype(jnp.int32)
    table = labels.reshape(top, rows).T
    table = table[jax.random.permutation(jax.random.fold_in(own, 1), rows)]
    turn = jax.random.randint(jax.random.fold_in(own, 2), (rows, 1), 0, top)
    return jnp.take_along_axis(table, (jnp.arange(top)[None, :] + turn) % top, axis=1)


def portions_of(count, total, limit, skew, full):
    weights = [(1 << 20) // math.isqrt(rank ** skew) + 1 for rank in range(1, count + 1)]
    largest = limit if full else min(limit, max(-(-total // count), total * weights[0] // sum(weights)))
    least = 1 if total - largest >= count - 1 else 0
    holding, spare = [largest] + [least] * (count - 1), total - largest - least * (count - 1)
    while spare > 0:
        candidates = [i for i in range(1, count) if holding[i] < largest] or [i for i in range(1, count) if holding[i] < limit]
        mass, left = sum([weights[i] for i in candidates]), spare
        for i in candidates:
            extra = min(limit - holding[i], max(1, left * weights[i] // mass), spare)
            holding[i] = holding[i] + extra
            spare = spare - extra
    return np.array(holding)


def noise(stream_key, dims, width, reach, shards=(), held_as=jnp.bfloat16):
    loudness = levels(stream_key, dims, shards, -0.22, 0.18) if shards else 1.0
    array = jax.random.normal(stream_key, dims, jnp.float32) * width * loudness
    return jnp.minimum(jnp.maximum(array, -reach), reach).astype(held_as)


def setup_inputs(seed: int = 0) -> dict:
    keys = jax.random.split(jax.random.key(seed), 11)
    pressure_start = noise(keys[0], (NX, NY, NZ), 1.0, 6.0, ((0, 16), (1, 4), (2, 4)), jnp.float32)
    saturation = jnp.clip(0.1 + 0.79999997 * jax.random.uniform(keys[1], (NX, NY, NZ), jnp.float32) ** levels(keys[1], (NX, NY, NZ), ((0, 16), (1, 4), (2, 4)), -0.2, 0.2), 0.1, 0.9)
    permeability = jnp.clip(jnp.exp(math.log(10.0) - 4.6051702 * jax.random.uniform(keys[2], (NX, NY, NZ), jnp.float32) ** levels(keys[2], (NX, NY, NZ), ((0, 16), (1, 4), (2, 4)), -0.2, 0.2)), 0.1, 10.0)
    rock_type = set_ends(jax.random.randint(keys[3], (NX, NY, NZ), 0, ROCKS), jax.random.fold_in(keys[3], 1), 0, ROCKS - 1).astype(jnp.int32)
    rock_table = jnp.clip(jax.random.uniform(keys[4], (5, ROCKS), jnp.float32, 0.5, 3.0), 0.5, 3.0)
    well_cells = set_ends(jax.random.randint(keys[5], (WELLS,), 0, NX * NY * NZ), jax.random.fold_in(keys[5], 1), 0, (NX * NY * NZ) - 1).astype(jnp.int32)
    well_rates = noise(keys[6], (WELLS,), 3.0, 12.0, (), jnp.float32)
    owner_map_keys = jax.random.split(jax.random.fold_in(keys[7], 1), SLABS_X * SLABS_Y * LAYERS_Z * BRICKS // BRICKS)
    owner_map_turns = jax.random.permutation(jax.random.fold_in(keys[7], 3), SLABS_X * SLABS_Y * LAYERS_Z * BRICKS // BRICKS)
    owner_map = jax.vmap(lambda own, number: assign_block(jax.random.fold_in(keys[7], 2), own, number, BRICKS, SLABS_X, 1, CAP, 2))(owner_map_keys, owner_map_turns).reshape((SLABS_X, SLABS_Y, LAYERS_Z, BRICKS, 1))
    stiffness = draw_stiffness(jax.random.fold_in(keys[10], 71), 0)
    anchored = set_ends((jax.random.randint(keys[9], (NX, NY, NZ), 0, 24) < 1).astype(jnp.int32), jax.random.fold_in(keys[9], 1), 0, 1)
    return {"pressure_start": pressure_start, "saturation": saturation, "permeability": permeability, "rock_type": rock_type, "rock_table": rock_table, "well_cells": well_cells, "well_rates": well_rates, "owner_map": owner_map, "stiffness": stiffness, "anchored": anchored}


OMEGA = 0.6
OFFSETS = tuple((along_x, along_y, along_z) for along_x in (0, 1) for along_y in (0, 1) for along_z in (0, 1))


def corner_signs():
    sign_table = np.zeros((24,), np.float32)
    for comp_idx in range(3):
        for corner_idx, offset in enumerate(OFFSETS):
            sign_table[comp_idx * 8 + corner_idx] = 0.25 * (2 * offset[comp_idx] - 1)
    return jnp.asarray(sign_table)


def rock_values(rock_type, rock_table):
    rock_ids = jnp.arange(rock_table.shape[1], dtype=jnp.int32)
    one_hot = (rock_type[None] == rock_ids[:, None, None, None]).astype(jnp.float32)
    return jnp.tensordot(rock_table, one_hot, 1, precision=lax.Precision.HIGHEST)


def transmit(left_value, right_value):
    summed = left_value + right_value
    return 2.0 * left_value * right_value / jnp.where(summed > 0, summed, 1.0)


def neighbour_view(values, axis_dim, shift_by):
    starts = [1, 1, 1]
    starts[axis_dim] = 1 + shift_by
    finish = [starts[0] + values.shape[0] - 2, starts[1] + values.shape[1] - 2, starts[2] + values.shape[2] - 2]
    return lax.slice(values, starts, finish)


def relax_cells(padded_p, padded_k, numerator, denominator):
    centre = padded_k[1:-1, 1:-1, 1:-1]
    total_num = numerator
    total_den = denominator
    for axis_dim in range(3):
        for shift_by in (-1, 1):
            trans = transmit(centre, neighbour_view(padded_k, axis_dim, shift_by))
            total_num = total_num + trans * neighbour_view(padded_p, axis_dim, shift_by)
            total_den = total_den + trans
    return total_num / total_den


def pad_cells(values):
    values = jnp.pad(values, ((1, 1), (0, 0), (0, 0)), mode="wrap")
    return jnp.pad(values, ((0, 0), (1, 1), (1, 1)))


def gather_nodes(nodes):
    pieces = []
    for offset in OFFSETS:
        rolled = jnp.roll(nodes, -offset[0], axis=1)
        pieces.append(rolled[:, :, offset[1]:offset[1] + NY, offset[2]:offset[2] + NZ])
    stacked = jnp.stack(pieces, axis=1)
    return stacked.reshape((stacked.shape[0] * 8,) + stacked.shape[2:])


def spread_nodes(element):
    comps = element.shape[0] // 8
    shaped = element.reshape((comps, 8) + element.shape[1:])
    summed = jnp.zeros((comps, NX, NY + 1, NZ + 1), jnp.float32)
    for corner_idx, offset in enumerate(OFFSETS):
        padded = jnp.pad(shaped[:, corner_idx], ((0, 0), (0, 0), (offset[1], 1 - offset[1]), (offset[2], 1 - offset[2])))
        summed = summed + jnp.roll(padded, offset[0], axis=1)
    return summed


def brick_blocks(owner_map, stiffness):
    owners = owner_map[..., 0]
    one_hot = (owners[..., None] == jnp.arange(N_GX, dtype=jnp.int32)).astype(jnp.int32)
    before = jnp.cumsum(one_hot, axis=3) - one_hot
    brick_rank = jnp.sum(before * one_hot, axis=-1).astype(jnp.int32)
    source_x = jnp.arange(N_GX, dtype=jnp.int32)[:, None, None, None]
    index_y = jnp.arange(N_GY, dtype=jnp.int32)[None, :, None, None]
    index_z = jnp.arange(N_GRP, dtype=jnp.int32)[None, None, :, None]
    picked = stiffness[owners, index_y, index_z, source_x, brick_rank]
    picked = picked.reshape(N_GX, N_GY, N_GRP, CX, CY, 24, 24)
    picked = picked.transpose(0, 3, 1, 4, 2, 5, 6)
    return picked.reshape(NX, NY, N_GRP, 24, 24)


def element_products(blocks, rounded):
    shaped = rounded.reshape(24, NX, NY, N_GRP, CZ).transpose(1, 2, 3, 0, 4).astype(jnp.float32)
    result = jnp.einsum("xygrc,xygcz->xygrz", blocks.astype(jnp.float32), shaped, precision=lax.Precision.HIGHEST)
    return result.transpose(3, 0, 1, 2, 4).reshape(24, NX, NY, NZ)


def reference(pressure_start, saturation, permeability, rock_type, rock_table, well_cells, well_rates, owner_map, stiffness, anchored):
    rock_props = rock_values(rock_type, rock_table)
    mobility = jnp.exp(rock_props[0] * jnp.log(saturation)) + 2.0 * jnp.exp(rock_props[1] * jnp.log(1.0 - saturation))
    conductance = permeability * mobility
    storage = rock_props[2]
    stress_term = rock_props[3]
    biot_coef = rock_props[4]
    source = jnp.zeros((NX * NY * NZ,), jnp.float32).at[well_cells].add(well_rates).reshape(NX, NY, NZ)
    base_term = storage * pressure_start + source
    padded_k = pad_cells(conductance)
    blocks = brick_blocks(owner_map, stiffness)
    diag_brick = jnp.diagonal(blocks.astype(jnp.float32), axis1=3, axis2=4)
    diag_elem = jnp.broadcast_to(diag_brick.transpose(3, 0, 1, 2)[..., None], (24, NX, NY, N_GRP, CZ)).reshape(24, NX, NY, NZ)
    node_diag = spread_nodes(diag_elem)
    anchor_elem = jnp.broadcast_to(anchored.astype(jnp.float32)[None], (8, NX, NY, NZ))
    free_nodes = jnp.where(spread_nodes(anchor_elem) > 0, 0.0, 1.0).astype(jnp.float32)
    corner_sign = corner_signs()
    displacement = jnp.zeros((3, NX, NY + 1, NZ + 1), jnp.float32)
    strain = jnp.zeros((NX, NY, NZ), jnp.float32)
    pressure = pressure_start
    for outer_step in range(ITERS):
        anchor = pressure
        numerator = base_term + stress_term * anchor - biot_coef * strain
        denominator = storage + stress_term
        for flow_step in range(FLOW_PASSES):
            pressure = relax_cells(pad_cells(pressure), padded_k, numerator, denominator)
        biot_load = (biot_coef * pressure)[None] * corner_sign[:, None, None, None]
        for mech_step in range(MECH_PASSES):
            corner_u = gather_nodes(displacement)
            rounded = corner_u.astype(jnp.bfloat16)
            element_force = element_products(blocks, rounded)
            residual = spread_nodes(biot_load - element_force)
            displacement = free_nodes * (displacement + OMEGA * residual / node_diag)
        strain = jnp.tensordot(corner_sign, gather_nodes(displacement), 1, precision=lax.Precision.HIGHEST)
    return pressure, strain
```

```python
import jax
import jax.numpy as jnp
import numpy as np
from jax import lax
from jax.sharding import Mesh
from jax.sharding import PartitionSpec as P

ITERS = 2
FLOW_PASSES = 4
MECH_PASSES = 3
OMEGA = 0.6
GX = ("gx_0", "gx_1", "gx_2")
BF = jnp.bfloat16
F32 = jnp.float32
RIM = 8
ZRIM = 14
ZR1 = 7
ERIM = 3


def row_order():
    order = np.zeros((32, 24), np.float32)
    sign = np.zeros((2, 2, 8), np.float32)
    for c in range(3):
        for dx in (0, 1):
            for dy in (0, 1):
                for dz in (0, 1):
                    order[8 * (2 * dx + dy) + 4 * dz + c, 8 * c + 4 * dx + 2 * dy + dz] = 1.0
                    sign[dx, dy, 4 * dz + c] = 0.25 * (2 * (dx, dy, dz)[c] - 1)
    return order, sign


def exchange(to_low, to_high, axis, periodic):
    count = lax.axis_size(axis)
    last = count if periodic else count - 1
    up = [(i, (i + 1) % count) for i in range(last)]
    down = [((i + 1) % count, i) for i in range(last)]
    return lax.ppermute(to_high, axis, up), lax.ppermute(to_low, axis, down)


def rows_of(*parts):
    return jnp.concatenate([p.reshape(-1, 128) for p in parts], axis=0)


def cut_rows(buffer, shapes):
    out, at = [], 0
    for shape in shapes:
        rows = int(np.prod(shape)) // 128
        out.append(buffer[at : at + rows].reshape(shape))
        at += rows
    return out


def lane_pad(a):
    return jnp.pad(a, [(0, 0)] * (a.ndim - 1) + [(0, 128 - a.shape[-1])])


def cut_along(array, dim, peers):
    lengths = array.shape
    parts = array.reshape(*lengths[:dim], peers, lengths[dim] // peers, *lengths[dim + 1 :])
    return jnp.moveaxis(parts, dim, 0)


def joined_along(parts, dim):
    lengths = list(parts.shape[1:])
    lengths[dim] *= parts.shape[0]
    return jnp.moveaxis(parts, 0, dim).reshape(lengths)


def exchange_in_order(parts, axes, order):
    lengths = [lax.axis_size(a) for a in axes]
    parts = parts.reshape(*lengths, *parts.shape[1:])
    for k in order:
        parts = lax.all_to_all(parts, axes[k], split_axis=k, concat_axis=k, tiled=True)
    return parts.reshape(-1, *parts.shape[len(axes) :])


def core_and_chips(array, groups, order, split_dim, concat_dim):
    peers = lax.axis_size(groups[0]) * lax.axis_size(groups[1])
    parts = cut_along(array, split_dim, peers)
    return joined_along(exchange_in_order(parts, groups, order), concat_dim)


def pick(rock, table, row):
    value = jnp.full(rock.shape, table[row, 0], F32)
    for k in range(1, table.shape[1]):
        value = jnp.where(rock == k, table[row, k], value)
    return value


def transmit(a, b):
    total = a + b
    return 2.0 * a * b / jnp.where(total > 0, total, 1.0)


def up_y(a):
    return jnp.pad(a[:, 1:], ((0, 0), (0, 1), (0, 0)))


def down_y(a):
    return jnp.pad(a[:, :-1], ((0, 0), (1, 0), (0, 0)))


def up_z(a):
    return jnp.roll(a, -1, axis=-1)


def down_z(a):
    return jnp.roll(a, 1, axis=-1)


def fold_z(g):
    swapped = jnp.roll(g, 4, axis=2)
    row = lax.broadcasted_iota(jnp.int32, g.shape, 2)
    return g + jnp.where(row < 4, down_z(swapped), up_z(swapped))


def spread(parts):
    nx, ny = parts[0][0].shape[0] - 1, parts[0][0].shape[1] - 1
    total = None
    for dx in (0, 1):
        for dy in (0, 1):
            a = parts[dx][dy]
            term = a[1 - dx : 1 - dx + nx, 1 - dy : 1 - dy + ny]
            total = term if total is None else total + term
    return total


def per_device(
    pressure_start,
    saturation,
    permeability,
    rock_type,
    rock_table,
    well_cells,
    well_rates,
    owner_map,
    stiffness,
    anchored,
):
    cx, cy, cz = pressure_start.shape
    count_x = lax.axis_size(GX)
    total_x = cx * count_x
    total_y = cy * lax.axis_size("gy")
    total_z = cz * lax.axis_size("grp")
    start_x = lax.axis_index(GX) * cx
    start_y = lax.axis_index("gy") * cy
    start_z = lax.axis_index("grp") * cz
    order, sign = row_order()
    ex, ey = cx + 2 * RIM, cy + 2 * RIM

    owners = owner_map.reshape(-1)
    capacity = stiffness.shape[4]
    one_hot = (owners[:, None] == jnp.arange(count_x, dtype=jnp.int32)[None, :]).astype(jnp.int32)
    before = jnp.cumsum(one_hot, axis=0) - one_hot
    brick_rank = jnp.sum(before * one_hot, axis=1)
    slot_index = owners * capacity + brick_rank
    held_blocks = stiffness.reshape(count_x, capacity, 24, 24)
    fetched = core_and_chips(held_blocks, (("gx_0", "gx_1"), "gx_2"), (1, 0), 0, 0)
    brick_k = fetched.reshape(count_x * capacity, 24, 24)[slot_index]
    perm = jnp.asarray(order, BF)
    half = jnp.einsum("brk,ck->brc", brick_k, perm, preferred_element_type=F32).astype(BF)
    block = jnp.einsum("ar,brc->bac", perm, half, preferred_element_type=F32).astype(BF)
    block = block.reshape(cx, cy, 32, 32)

    mobility = jnp.exp(pick(rock_type, rock_table, 0) * jnp.log(saturation)) + 2.0 * jnp.exp(
        pick(rock_type, rock_table, 1) * jnp.log(1.0 - saturation)
    )
    conductance = permeability * mobility
    fields = [a.astype(BF) for a in (pressure_start, conductance, rock_type, anchored)]

    def k_lanes(b):
        return lane_pad(jnp.concatenate([b[:, i] for i in range(ERIM)], axis=-1))

    got = exchange(
        rows_of(*fields, k_lanes(block[:, :ERIM])),
        rows_of(*fields, k_lanes(block[:, cy - ERIM :])),
        "gy",
        False,
    )
    shapes = [(cx, cy, cz)] * 4 + [(cx, 32, 128)]
    low, high = cut_rows(got[0], shapes), cut_rows(got[1], shapes)
    fields = [jnp.concatenate([low[i], fields[i], high[i]], axis=1) for i in range(4)]

    def k_apart(lanes):
        return jnp.stack([lanes[:, :, 32 * i : 32 * i + 32] for i in range(ERIM)], axis=1)

    block = jnp.concatenate([k_apart(low[4]), block, k_apart(high[4])], axis=1)
    ky = cy + 2 * ERIM

    quad = block.reshape(2, 4, ky, 32, 32)
    quad = jnp.concatenate([quad[:, i] for i in range(4)], axis=-1)
    got = exchange(
        rows_of(lane_pad(jnp.concatenate([f[..., :ZRIM] for f in fields], axis=-1)), quad),
        rows_of(lane_pad(jnp.concatenate([f[..., cz - ZRIM :] for f in fields], axis=-1)), quad),
        "grp",
        False,
    )
    shapes = [(cx, ey, 128), (2, ky, 32, 128)]
    low, high = cut_rows(got[0], shapes), cut_rows(got[1], shapes)
    ends = lane_pad(jnp.concatenate([high[0][..., : 4 * ZRIM], low[0][..., : 4 * ZRIM]], axis=-1))

    def quad_apart(q):
        return jnp.stack([q[..., 32 * i : 32 * i + 32] for i in range(4)], axis=1).reshape(cx, ky, 32, 32)

    block = lane_pad(jnp.concatenate([block, quad_apart(high[1]), quad_apart(low[1])], axis=-1))

    got = exchange(
        rows_of(*fields, ends, block[:ERIM]),
        rows_of(*fields, ends, block[cx - ERIM :]),
        GX,
        True,
    )
    shapes = [(cx, ey, 128)] * 5 + [(ERIM, ky, 32, 128)]
    low, high = cut_rows(got[0], shapes), cut_rows(got[1], shapes)
    fields = [jnp.concatenate([low[i], fields[i], high[i]], axis=0) for i in range(4)]
    ends = jnp.concatenate([low[4], ends, high[4]], axis=0)
    block = jnp.concatenate([low[5], block, high[5]], axis=0)
    gap = jnp.zeros((ex, ey, 128 - 2 * ZRIM), BF)

    def whole(i):
        after = ends[..., i * ZRIM : (i + 1) * ZRIM]
        ahead = ends[..., (4 + i) * ZRIM : (5 + i) * ZRIM]
        return jnp.concatenate([fields[i], after, gap, ahead], axis=-1).astype(F32)

    def with_own(ext, own):
        return lax.dynamic_update_slice(ext, own, (RIM, RIM, 0))

    p_start = with_own(whole(0), pressure_start)
    cond = with_own(whole(1), conductance)
    rock = whole(2)
    held = whole(3)[RIM - ERIM : RIM + cx + ERIM, RIM - ERIM : RIM + cy + ERIM]

    storage = pick(rock, rock_table, 2)
    stress = pick(rock, rock_table, 3)
    place = lax.broadcasted_iota(jnp.int32, (1, 1, 256), 2)
    place = jnp.where(place < 192, place, place - 256) + start_z
    biot = jnp.where((place >= 0) & (place < total_z), pick(rock, rock_table, 4), 0.0)
    plane = total_y * total_z
    well_x = (well_cells // plane - start_x + RIM) % total_x
    well_y = well_cells // total_z % total_y - start_y + RIM
    well_z = well_cells % total_z - start_z
    near = (well_z >= -ZRIM) & (well_z < cz + ZRIM)
    lane = jnp.where(near, well_z % 256, -1)
    at_x = (jnp.arange(ex, dtype=jnp.int32)[:, None] == well_x[None, :]).astype(F32)
    at_y = (jnp.arange(ey, dtype=jnp.int32)[:, None] == well_y[None, :]).astype(F32)
    at_xy = (at_x[:, None, :] * at_y[None, :, :]).reshape(ex * ey, -1)
    at_z = jnp.where(lane[:, None] == jnp.arange(256, dtype=jnp.int32)[None, :], well_rates[:, None], 0.0)
    source = jnp.dot(at_xy, at_z, precision=lax.Precision.HIGHEST).reshape(ex, ey, 256)
    base = storage * p_start + source
    tx = transmit(cond[:-1], cond[1:])
    ty = transmit(cond, up_y(cond))
    tz = transmit(cond, up_z(cond))
    ty_low, tz_low = down_y(ty), down_z(tz)
    inner = slice(1, ex - 1)
    den = (storage + stress + ty + ty_low + tz + tz_low)[inner] + tx[:-1] + tx[1:]
    inv_den = 1.0 / den

    def flow(anchor, numerator):
        current = anchor
        for k in range(1, FLOW_PASSES + 1):
            lo, hi = 1 + k, ex - 1 - k
            n = hi - lo
            off = 1 if k == 1 else 0
            mid = current[1 + off : 1 + off + n]
            total = (
                numerator[lo:hi]
                + tx[lo - 1 : hi - 1] * current[off : off + n]
                + tx[lo:hi] * current[2 + off : 2 + off + n]
                + ty[lo:hi] * up_y(mid)
                + ty_low[lo:hi] * down_y(mid)
                + tz[lo:hi] * up_z(mid)
                + tz_low[lo:hi] * down_z(mid)
            )
            current = total * inv_den[lo - 1 : hi - 1]
        return current

    z_lane = lax.broadcasted_iota(jnp.int32, (1, 1, 1, 256), 3)
    eye = jnp.asarray(np.tile(np.eye(32, dtype=np.float32), (1, 4))[:, :128])
    diag = block.astype(F32) * eye
    d_own, d_next, d_prev = (jnp.sum(diag[..., 32 * i : 32 * i + 32], axis=-1, keepdims=True) for i in range(3))
    diag = jnp.where(z_lane < 128, d_own, jnp.where(z_lane < 192, d_next, d_prev))

    def quarters(a):
        return [[a[:, :, 8 * (2 * dx + dy) : 8 * (2 * dx + dy) + 8] for dy in (0, 1)] for dx in (0, 1)]

    node_diag = fold_z(spread(quarters(diag)))
    fixed = held[:-1, :-1] + held[1:, :-1] + held[:-1, 1:] + held[1:, 1:]
    fixed = (fixed + down_z(fixed))[:, :, None, :]
    row8 = lax.broadcasted_iota(jnp.int32, (1, 1, 8, 256), 2)
    fixed = jnp.where(row8 < 4, fixed, up_z(fixed))
    free = jnp.where(fixed > 0, 0.0, 1.0)
    step = jnp.where(node_diag > 0, OMEGA * free / jnp.where(node_diag > 0, node_diag, 1.0), 0.0)
    k_own = block[..., :32]
    k_ends = block[..., 32:96]
    signs = jnp.asarray(sign)

    def load_of(pressure):
        m = RIM - ERIM
        bp = (biot[m : ex - m] * pressure)[:, m : ey - m][:, :, None, :]
        return fold_z(spread([[bp * signs[dx, dy][None, None, :, None] for dy in (0, 1)] for dx in (0, 1)]))

    def force_of(disp, rim):
        n, m = cx + 2 * rim, ERIM - rim
        u = disp.astype(BF)
        u = jnp.concatenate([u[dx : dx + n, dy : dy + n] for dx in (0, 1) for dy in (0, 1)], axis=2)
        ends_u = u[..., 128:]
        lanes = lax.broadcasted_iota(jnp.int32, ends_u.shape, 3)
        ends_u = jnp.concatenate(
            [jnp.where(lanes < 64, ends_u, 0), jnp.where(lanes >= 64, ends_u, 0)], axis=2
        )
        ko = k_own[m : m + n, m : m + n]
        ke = k_ends[m : m + n, m : m + n]
        f_own = jnp.einsum("xyrk,xykz->xyrz", ko, u[..., :128], preferred_element_type=F32)
        f_end = jnp.einsum("xyrk,xykz->xyrz", ke, ends_u, preferred_element_type=F32)
        return fold_z(spread(quarters(jnp.concatenate([f_own, f_end], axis=-1))))

    def mech(load, disp):
        for k in range(MECH_PASSES):
            m = k
            n = cx + 1 + 2 * (ERIM - 1 - k)
            cut = (slice(m, m + n), slice(m, m + n))
            if disp is None:
                disp = step[cut] * load[cut]
            else:
                residual = load[cut] - force_of(disp, ERIM - k)
                disp = free[cut] * disp[1:-1, 1:-1] + step[cut] * residual
        return disp

    def strain_of(disp):
        total = 0.0
        for dx in (0, 1):
            for dy in (0, 1):
                total = total + disp[dx : dx + cx, dy : dy + cy] * signs[dx, dy][None, None, :, None]
        return jnp.sum(total, axis=2)

    p1 = flow(p_start, base + stress * p_start)
    d1 = mech(load_of(p1), None)
    s1 = strain_of(d1)
    p1 = p1[ERIM : ERIM + cx, RIM : RIM + cy]

    def ends_of(a):
        return jnp.concatenate([a[..., 128 : 128 + ZR1], a[..., 256 - ZR1 :]], axis=-1)

    p_bf, s_bf = p1.astype(BF), s1.astype(BF)
    moving = [p_bf[..., :128], s_bf[..., :128], lane_pad(jnp.concatenate([ends_of(p_bf), ends_of(s_bf)], axis=-1))]
    d_pack = jnp.concatenate([d1[:, :, :4, :128], d1[:, :, :4, 128:]], axis=2)
    d_bf = d_pack.astype(BF)
    got = exchange(
        rows_of(*moving, d_bf[:, 1 : 1 + ERIM]),
        rows_of(*moving, d_bf[:, cy - ERIM : cy]),
        "gy",
        False,
    )
    shapes = [(cx, cy, 128)] * 3 + [(cx + 1, ERIM, 8, 128)]
    low, high = cut_rows(got[0], shapes), cut_rows(got[1], shapes)
    moving = [jnp.concatenate([low[i], moving[i], high[i]], axis=1) for i in range(3)]
    d_bf = jnp.concatenate([low[3], d_bf, high[3]], axis=1)
    got = exchange(
        rows_of(*moving, d_bf[1 : 1 + ERIM]),
        rows_of(*moving, d_bf[cx - ERIM : cx]),
        GX,
        True,
    )
    shapes = [(cx, ey, 128)] * 3 + [(ERIM, cy + 1 + 2 * ERIM, 8, 128)]
    low, high = cut_rows(got[0], shapes), cut_rows(got[1], shapes)
    moving = [jnp.concatenate([low[i], moving[i], high[i]], axis=0) for i in range(3)]
    d_bf = jnp.concatenate([low[3], d_bf, high[3]], axis=0)
    gap = jnp.zeros((ex, ey, 128 - 2 * ZR1), BF)

    def whole_again(i, own):
        after = moving[2][..., 2 * i * ZR1 : (2 * i + 1) * ZR1]
        ahead = moving[2][..., (2 * i + 1) * ZR1 : (2 * i + 2) * ZR1]
        return with_own(jnp.concatenate([moving[i], after, gap, ahead], axis=-1).astype(F32), own)

    p_ext = whole_again(0, p1)
    s_ext = whole_again(1, s1)
    d_ext = lax.dynamic_update_slice(d_bf.astype(F32), d_pack, (ERIM, ERIM, 0, 0))
    d_ext = jnp.concatenate([d_ext[:, :, :4], d_ext[:, :, 4:]], axis=-1)
    d_ext = jnp.concatenate([d_ext, up_z(d_ext)], axis=2)

    p2 = flow(p_ext, base + stress * p_ext - biot * s_ext)
    load = load_of(p2)
    disp = d_ext
    disp = mech(load, disp)
    strain = strain_of(disp)[..., :128]
    return (p2[ERIM : ERIM + cx, RIM : RIM + cy, :128], strain)


def solution(mesh):
    torus = Mesh(
        mesh.devices.reshape(mesh.shape["grp"], 4, 2, 2, mesh.shape["gy"]),
        ("grp", "gx_0", "gx_1", "gx_2", "gy"),
    )
    return jax.shard_map(
        per_device,
        mesh=torus,
        in_specs=(
            P(GX, "gy", "grp"),
            P(GX, "gy", "grp"),
            P(GX, "gy", "grp"),
            P(GX, "gy", "grp"),
            P(),
            P(),
            P(),
            P(GX, "gy", "grp", None, None),
            P(GX, "gy", "grp", None, None, None, None),
            P(GX, "gy", "grp"),
        ),
        out_specs=(P(GX, "gy", "grp"), P(GX, "gy", "grp")),
        check_vma=False,
    )
```

```python
import jax
import jax.numpy as jnp
import numpy as np
from jax import lax
from jax.experimental import pallas as pl
from jax.experimental.pallas import tpu as pltpu
from jax.sharding import Mesh
from jax.sharding import PartitionSpec as P

ITERS = 2
FLOW_PASSES = 4
MECH_PASSES = 3
OMEGA = 0.6
GX = ("gx_0", "gx_1", "gx_2")
BF = jnp.bfloat16
F32 = jnp.float32
RIM = 8
ZRIM = 14
ZR1 = 7
ERIM = 3


def row_order():
    order = np.zeros((32, 24), np.float32)
    sign = np.zeros((2, 2, 8), np.float32)
    for c in range(3):
        for dx in (0, 1):
            for dy in (0, 1):
                for dz in (0, 1):
                    order[8 * (2 * dx + dy) + 4 * dz + c, 8 * c + 4 * dx + 2 * dy + dz] = 1.0
                    sign[dx, dy, 4 * dz + c] = 0.25 * (2 * (dx, dy, dz)[c] - 1)
    return order, sign


def exchange(to_low, to_high, axis, periodic):
    count = lax.axis_size(axis)
    last = count if periodic else count - 1
    up = [(i, (i + 1) % count) for i in range(last)]
    down = [((i + 1) % count, i) for i in range(last)]
    return lax.ppermute(to_high, axis, up), lax.ppermute(to_low, axis, down)


def rows_of(*parts):
    return jnp.concatenate([p.reshape(-1, 128) for p in parts], axis=0)


def cut_rows(buffer, shapes):
    out, at = [], 0
    for shape in shapes:
        rows = int(np.prod(shape)) // 128
        out.append(buffer[at : at + rows].reshape(shape))
        at += rows
    return out


def lane_pad(a):
    return jnp.pad(a, [(0, 0)] * (a.ndim - 1) + [(0, 128 - a.shape[-1])])


def cut_along(array, dim, peers):
    lengths = array.shape
    parts = array.reshape(*lengths[:dim], peers, lengths[dim] // peers, *lengths[dim + 1 :])
    return jnp.moveaxis(parts, dim, 0)


def joined_along(parts, dim):
    lengths = list(parts.shape[1:])
    lengths[dim] *= parts.shape[0]
    return jnp.moveaxis(parts, 0, dim).reshape(lengths)


def exchange_in_order(parts, axes, order):
    lengths = [lax.axis_size(a) for a in axes]
    parts = parts.reshape(*lengths, *parts.shape[1:])
    for k in order:
        parts = lax.all_to_all(parts, axes[k], split_axis=k, concat_axis=k, tiled=True)
    return parts.reshape(-1, *parts.shape[len(axes) :])


def core_and_chips(array, groups, order, split_dim, concat_dim):
    peers = lax.axis_size(groups[0]) * lax.axis_size(groups[1])
    parts = cut_along(array, split_dim, peers)
    return joined_along(exchange_in_order(parts, groups, order), concat_dim)


def pick(rock, table):
    one_hot = (rock[None] == jnp.arange(table.shape[1], dtype=jnp.int32)[:, None, None, None]).astype(F32)
    return jnp.tensordot(table, one_hot, 1, precision=lax.Precision.HIGHEST)


def transmit(a, b):
    total = a + b
    return 2.0 * a * b / jnp.where(total > 0, total, 1.0)


def up_y(a):
    return jnp.pad(a[:, 1:], ((0, 0), (0, 1), (0, 0)))


def down_y(a):
    return jnp.pad(a[:, :-1], ((0, 0), (1, 0), (0, 0)))


def up_z(a):
    return jnp.roll(a, -1, axis=-1)


def down_z(a):
    return jnp.roll(a, 1, axis=-1)


def fold_z(g):
    swapped = jnp.roll(g, 4, axis=2)
    row = lax.broadcasted_iota(jnp.int32, g.shape, 2)
    return g + jnp.where(row < 4, down_z(swapped), up_z(swapped))


def spread(parts):
    nx, ny = parts[0][0].shape[0] - 1, parts[0][0].shape[1] - 1
    total = None
    for dx in (0, 1):
        for dy in (0, 1):
            a = parts[dx][dy]
            term = a[1 - dx : 1 - dx + nx, 1 - dy : 1 - dy + ny]
            total = term if total is None else total + term
    return total


def roll_up(a, axis):
    return pltpu.roll(a, a.shape[axis] - 1, axis)


def roll_down(a, axis):
    return pltpu.roll(a, 1, axis)


def flow_passes(start, spare, num, tx, ty, ty_low, tz, tz_low, inv_den, out):
    ex = start.shape[0]
    for k in range(1, FLOW_PASSES + 1):
        src = start if k % 2 == 1 else spare
        dst = spare if k % 2 == 1 else start
        lo, hi = 1 + k, ex - 1 - k

        def step(x, carry):
            mid = src[x]
            total = (
                (num[x] + tx[x - 1] * src[x - 1])
                + (tx[x] * src[x + 1] + ty[x] * roll_up(mid, 0))
                + (ty_low[x] * roll_down(mid, 0) + tz[x] * roll_up(mid, 1))
                + tz_low[x] * roll_down(mid, 1)
            ) * inv_den[x]
            if k == FLOW_PASSES:
                out[x - lo] = total
            else:
                dst[x] = total
            return carry

        lax.fori_loop(lo, hi, step, 0, unroll=2)


def first_flow(
    table, z_range, fp, fc, fr, ends, place, p_own, c_own, source,
    out, base, stress, biot, tx, ty, ty_low, tz, tz_low, inv_den,
    start, spare, cond, num,
):
    ex, ey = start.shape[0], start.shape[1]
    cx = p_own.shape[0]
    lane = lax.broadcasted_iota(jnp.int32, (ey, 256), 1)
    z_at = jnp.where(lane < 192, lane, lane - 256) + z_range[0]
    z_in = (z_at >= 0) & (z_at < z_range[1])

    def choose(rock, row):
        value = jnp.full(rock.shape, table[row, 3], F32)
        for r in range(3):
            value = jnp.where(rock == float(r), table[row, r], value)
        return value

    def gather(x, carry):
        apart = jnp.dot(ends[x], place[...], preferred_element_type=F32)
        start[x] = jnp.concatenate([fp[x].astype(F32), apart[:, :128]], axis=1)
        cond[x] = jnp.concatenate([fc[x].astype(F32), apart[:, 128:256]], axis=1)
        rock = jnp.concatenate([fr[x].astype(F32), apart[:, 256:]], axis=1)
        storage = choose(rock, 2)
        strained = choose(rock, 3)
        base[x] = storage
        stress[x] = strained
        biot[x] = jnp.where(z_in, choose(rock, 4), 0.0)
        inv_den[x] = storage + strained
        return carry

    lax.fori_loop(0, ex, gather, 0, unroll=2)
    start[RIM : RIM + cx, RIM : RIM + p_own.shape[1], 0:128] = p_own[...]
    cond[RIM : RIM + cx, RIM : RIM + p_own.shape[1], 0:128] = c_own[...]

    def static_terms(x, carry):
        c = cond[x]
        tx[x] = transmit(c, cond[jnp.minimum(x + 1, ex - 1)])
        t = transmit(c, roll_up(c, 0))
        low = roll_down(t, 0)
        ty[x] = t
        ty_low[x] = low
        den = inv_den[x] + t + low
        t = transmit(c, roll_up(c, 1))
        low = roll_down(t, 1)
        tz[x] = t
        tz_low[x] = low
        p = start[x]
        b = base[x] * p + source[x]
        base[x] = b
        num[x] = b + stress[x] * p
        inv_den[x] = 1.0 / (den + t + low + tx[x] + tx[jnp.maximum(x - 1, 0)])
        return carry

    lax.fori_loop(0, ex, static_terms, 0, unroll=2)
    flow_passes(start, spare, num, tx, ty, ty_low, tz, tz_low, inv_den, out)


def second_flow(
    fp, fs, ends, place, p_own, s_own, base, stress, biot, tx, ty, ty_low, tz, tz_low, inv_den,
    out, start, spare, num, strain,
):
    ex = start.shape[0]
    cx, cy = p_own.shape[0], p_own.shape[1]

    def gather(x, carry):
        apart = jnp.dot(ends[x], place[...], preferred_element_type=F32)
        start[x] = jnp.concatenate([fp[x].astype(F32), apart[:, :128]], axis=1)
        strain[x] = jnp.concatenate([fs[x].astype(F32), apart[:, 128:]], axis=1)
        return carry

    lax.fori_loop(0, ex, gather, 0, unroll=2)
    start[RIM : RIM + cx, RIM : RIM + cy, :] = p_own[...]
    strain[RIM : RIM + cx, RIM : RIM + cy, :] = s_own[...]

    def numerator(x, carry):
        num[x] = base[x] + stress[x] * start[x] - biot[x] * strain[x]
        return carry

    lax.fori_loop(2, ex - 2, numerator, 0, unroll=2)
    flow_passes(start, spare, num, tx, ty, ty_low, tz, tz_low, inv_den, out)


def vmem(n):
    return [pl.BlockSpec(memory_space=pltpu.VMEM)] * n


def end_places(count, width, fields):
    place = np.zeros((128, 128 * count), np.float32)
    for i in range(count):
        after, ahead = fields(i)
        for t in range(width):
            place[after + t, 128 * i + t] = 1.0
            place[ahead + t, 128 * i + 128 - width + t] = 1.0
    return jnp.asarray(place, BF)


def per_device(
    pressure_start,
    saturation,
    permeability,
    rock_type,
    rock_table,
    well_cells,
    well_rates,
    owner_map,
    stiffness,
    anchored,
):
    cx, cy, cz = pressure_start.shape
    count_x = lax.axis_size(GX)
    total_x = cx * count_x
    total_y = cy * lax.axis_size("gy")
    total_z = cz * lax.axis_size("grp")
    start_x = lax.axis_index(GX) * cx
    start_y = lax.axis_index("gy") * cy
    start_z = lax.axis_index("grp") * cz
    order, sign = row_order()
    ex, ey = cx + 2 * RIM, cy + 2 * RIM

    owners = owner_map.reshape(-1)
    capacity = stiffness.shape[4]
    one_hot = (owners[:, None] == jnp.arange(count_x, dtype=jnp.int32)[None, :]).astype(jnp.int32)
    before = jnp.cumsum(one_hot, axis=0) - one_hot
    brick_rank = jnp.sum(before * one_hot, axis=1)
    lanes_of = np.zeros((4, 24, 128), np.float32)
    for j in range(4):
        lanes_of[j, :, 32 * j : 32 * j + 32] = order.T
    lanes_of = jnp.asarray(lanes_of, BF)
    held_blocks = stiffness.reshape(count_x, capacity // 4, 4, 24, 24)
    packed = sum(
        jnp.einsum("ogrk,km->ogrm", held_blocks[:, :, j], lanes_of[j], preferred_element_type=F32) for j in range(4)
    ).astype(BF)
    fetched = core_and_chips(packed, (("gx_0", "gx_1"), "gx_2"), (1, 0), 0, 0)
    groups = fetched.reshape(count_x * (capacity // 4), 24, 128)[owners * (capacity // 4) + brick_rank // 4]
    lane_at = lax.broadcasted_iota(jnp.int32, groups.shape, 2) // 32
    groups = jnp.where(lane_at == (brick_rank % 4)[:, None, None], groups, 0)
    fold = jnp.asarray(np.tile(np.eye(32, dtype=np.float32), (4, 1)), BF)
    half = jnp.einsum("brm,mc->brc", groups, fold, preferred_element_type=F32).astype(BF)
    block = jnp.einsum("ar,brc->bac", jnp.asarray(order, BF), half, preferred_element_type=F32).astype(BF)
    block = block.reshape(cx, cy, 32, 32)

    exponents = pick(rock_type, rock_table[:2])
    mobility = jnp.exp(exponents[0] * jnp.log(saturation)) + 2.0 * jnp.exp(
        exponents[1] * jnp.log(1.0 - saturation)
    )
    conductance = permeability * mobility
    fields = [a.astype(BF) for a in (pressure_start, conductance, rock_type, anchored)]

    def k_lanes(b):
        return lane_pad(jnp.concatenate([b[:, i] for i in range(ERIM)], axis=-1))

    got = exchange(
        rows_of(*fields, k_lanes(block[:, :ERIM])),
        rows_of(*fields, k_lanes(block[:, cy - ERIM :])),
        "gy",
        False,
    )
    shapes = [(cx, cy, cz)] * 4 + [(cx, 32, 128)]
    low, high = cut_rows(got[0], shapes), cut_rows(got[1], shapes)
    fields = [jnp.concatenate([low[i], fields[i], high[i]], axis=1) for i in range(4)]

    def k_apart(lanes):
        return jnp.stack([lanes[:, :, 32 * i : 32 * i + 32] for i in range(ERIM)], axis=1)

    block = jnp.concatenate([k_apart(low[4]), block, k_apart(high[4])], axis=1)
    ky = cy + 2 * ERIM

    quad = block.reshape(2, 4, ky, 32, 32)
    quad = jnp.concatenate([quad[:, i] for i in range(4)], axis=-1)
    got = exchange(
        rows_of(lane_pad(jnp.concatenate([f[..., :ZRIM] for f in fields], axis=-1)), quad),
        rows_of(lane_pad(jnp.concatenate([f[..., cz - ZRIM :] for f in fields], axis=-1)), quad),
        "grp",
        False,
    )
    shapes = [(cx, ey, 128), (2, ky, 32, 128)]
    low, high = cut_rows(got[0], shapes), cut_rows(got[1], shapes)
    ends = lane_pad(jnp.concatenate([high[0][..., : 4 * ZRIM], low[0][..., : 4 * ZRIM]], axis=-1))

    def quad_apart(q):
        return jnp.stack([q[..., 32 * i : 32 * i + 32] for i in range(4)], axis=1).reshape(cx, ky, 32, 32)

    block = lane_pad(jnp.concatenate([block, quad_apart(high[1]), quad_apart(low[1])], axis=-1))

    got = exchange(
        rows_of(*fields, ends, block[:ERIM]),
        rows_of(*fields, ends, block[cx - ERIM :]),
        GX,
        True,
    )
    shapes = [(cx, ey, 128)] * 5 + [(ERIM, ky, 32, 128)]
    low, high = cut_rows(got[0], shapes), cut_rows(got[1], shapes)
    fields = [jnp.concatenate([low[i], fields[i], high[i]], axis=0) for i in range(4)]
    ends = jnp.concatenate([low[4], ends, high[4]], axis=0)
    block = jnp.concatenate([low[5], block, high[5]], axis=0)
    held = fields[3][RIM - ERIM : RIM + cx + ERIM, RIM - ERIM : RIM + cy + ERIM]
    held_ends = ends[RIM - ERIM : RIM + cx + ERIM, RIM - ERIM : RIM + cy + ERIM]
    held_place = end_places(1, ZRIM, lambda i: (3 * ZRIM, 7 * ZRIM))
    held_ends = jnp.einsum("xyl,lz->xyz", held_ends, held_place, preferred_element_type=F32)
    held = jnp.concatenate([held.astype(F32), held_ends], axis=-1)
    plane = total_y * total_z
    well_x = (well_cells // plane - start_x + RIM) % total_x
    well_y = well_cells // total_z % total_y - start_y + RIM
    well_z = well_cells % total_z - start_z
    near = (well_z >= -ZRIM) & (well_z < cz + ZRIM)
    lane = jnp.where(near, well_z % 256, -1)
    at_x = (jnp.arange(ex, dtype=jnp.int32)[:, None] == well_x[None, :]).astype(F32)
    at_y = (jnp.arange(ey, dtype=jnp.int32)[:, None] == well_y[None, :]).astype(F32)
    at_xy = (at_x[:, None, :] * at_y[None, :, :]).reshape(ex * ey, -1)
    at_z = jnp.where(lane[:, None] == jnp.arange(256, dtype=jnp.int32)[None, :], well_rates[:, None], 0.0)
    source = jnp.dot(at_xy, at_z, precision=lax.Precision.HIGHEST).reshape(ex, ey, 256)
    cells = jax.ShapeDtypeStruct((ex, ey, 256), F32)
    out = jax.ShapeDtypeStruct((cx + 2 * ERIM, ey, 256), F32)
    buf = pltpu.VMEM((ex, ey, 256), F32)
    z_range = jnp.stack([start_z, jnp.int32(total_z)]).astype(jnp.int32)
    p1, base, stress, biot, *links = pl.pallas_call(
        first_flow,
        out_shape=[out] + [cells] * 9,
        in_specs=[pl.BlockSpec(memory_space=pltpu.SMEM)] * 2 + vmem(8),
        out_specs=vmem(10),
        scratch_shapes=[buf] * 4,
        name="first_flow",
    )(
        rock_table, z_range, fields[0], fields[1], fields[2], ends,
        end_places(3, ZRIM, lambda i: (i * ZRIM, (4 + i) * ZRIM)), pressure_start, conductance, source,
    )

    z_lane = lax.broadcasted_iota(jnp.int32, (1, 1, 1, 256), 3)
    eye = np.tile(np.eye(32, dtype=np.float32), (1, 4))
    eye[:, 96:] = 0.0
    spans = np.zeros((128, 256), np.float32)
    spans[:32, :128] = 1.0
    spans[32:64, 128:192] = 1.0
    spans[64:96, 192:] = 1.0
    diag = block * jnp.asarray(eye, BF)
    diag = jnp.einsum("xyrk,kz->xyrz", diag, jnp.asarray(spans, BF), preferred_element_type=F32)

    def quarters(a):
        return [[a[:, :, 8 * (2 * dx + dy) : 8 * (2 * dx + dy) + 8] for dy in (0, 1)] for dx in (0, 1)]

    node_diag = fold_z(spread(quarters(diag)))
    fixed = held[:-1, :-1] + held[1:, :-1] + held[:-1, 1:] + held[1:, 1:]
    fixed = (fixed + down_z(fixed))[:, :, None, :]
    row8 = lax.broadcasted_iota(jnp.int32, (1, 1, 8, 256), 2)
    fixed = jnp.where(row8 < 4, fixed, up_z(fixed))
    free = jnp.where(fixed > 0, 0.0, 1.0)
    step = jnp.where(node_diag > 0, OMEGA * free / jnp.where(node_diag > 0, node_diag, 1.0), 0.0)
    k_own = block[..., :32]
    k_ends = jnp.concatenate([block[..., 32:64], block[..., 64:96]], axis=2)
    signs = jnp.asarray(sign)

    def load_of(pressure):
        m = RIM - ERIM
        bp = (biot[m : ex - m] * pressure)[:, m : ey - m][:, :, None, :]
        return fold_z(spread([[bp * signs[dx, dy][None, None, :, None] for dy in (0, 1)] for dx in (0, 1)]))

    def force_of(disp, rim):
        n, m = cx + 2 * rim, ERIM - rim
        u = disp.astype(BF)
        u = jnp.concatenate([u[dx : dx + n, dy : dy + n] for dx in (0, 1) for dy in (0, 1)], axis=2)
        ko = k_own[m : m + n, m : m + n]
        ke = k_ends[m : m + n, m : m + n]
        f_own = jnp.einsum("xyrk,xykz->xyrz", ko, u[..., :128], preferred_element_type=F32)
        f_end = jnp.einsum("xyrk,xykz->xyrz", ke, u[..., 128:], preferred_element_type=F32)
        f_end = jnp.where(z_lane[..., :128] < 64, f_end[:, :, :32], f_end[:, :, 32:])
        return fold_z(spread(quarters(jnp.concatenate([f_own, f_end], axis=-1))))

    def mech(load, disp):
        for k in range(MECH_PASSES):
            m = k
            n = cx + 1 + 2 * (ERIM - 1 - k)
            cut = (slice(m, m + n), slice(m, m + n))
            if disp is None:
                disp = step[cut] * load[cut]
            else:
                residual = load[cut] - force_of(disp, ERIM - k)
                disp = free[cut] * disp[1:-1, 1:-1] + step[cut] * residual
        return disp

    def strain_of(disp):
        total = 0.0
        for dx in (0, 1):
            for dy in (0, 1):
                total = total + disp[dx : dx + cx, dy : dy + cy] * signs[dx, dy][None, None, :, None]
        return jnp.sum(total, axis=2)

    d1 = mech(load_of(p1), None)
    s1 = strain_of(d1)
    p1 = p1[ERIM : ERIM + cx, RIM : RIM + cy]

    def ends_of(a):
        return jnp.concatenate([a[..., 128 : 128 + ZR1], a[..., 256 - ZR1 :]], axis=-1)

    p_bf, s_bf = p1.astype(BF), s1.astype(BF)
    moving = [p_bf[..., :128], s_bf[..., :128], lane_pad(jnp.concatenate([ends_of(p_bf), ends_of(s_bf)], axis=-1))]
    d_pack = jnp.concatenate([d1[:, :, :4, :128], d1[:, :, :4, 128:]], axis=2)
    d_bf = d_pack.astype(BF)
    got = exchange(
        rows_of(*moving, d_bf[:, 1 : 1 + ERIM]),
        rows_of(*moving, d_bf[:, cy - ERIM : cy]),
        "gy",
        False,
    )
    shapes = [(cx, cy, 128)] * 3 + [(cx + 1, ERIM, 8, 128)]
    low, high = cut_rows(got[0], shapes), cut_rows(got[1], shapes)
    moving = [jnp.concatenate([low[i], moving[i], high[i]], axis=1) for i in range(3)]
    d_bf = jnp.concatenate([low[3], d_bf, high[3]], axis=1)
    got = exchange(
        rows_of(*moving, d_bf[1 : 1 + ERIM]),
        rows_of(*moving, d_bf[cx - ERIM : cx]),
        GX,
        True,
    )
    shapes = [(cx, ey, 128)] * 3 + [(ERIM, cy + 1 + 2 * ERIM, 8, 128)]
    low, high = cut_rows(got[0], shapes), cut_rows(got[1], shapes)
    moving = [jnp.concatenate([low[i], moving[i], high[i]], axis=0) for i in range(3)]
    d_bf = jnp.concatenate([low[3], d_bf, high[3]], axis=0)
    d_ext = lax.dynamic_update_slice(d_bf.astype(F32), d_pack, (ERIM, ERIM, 0, 0))
    d_ext = jnp.concatenate([d_ext[:, :, :4], d_ext[:, :, 4:]], axis=-1)
    d_ext = jnp.concatenate([d_ext, up_z(d_ext)], axis=2)

    (p2,) = pl.pallas_call(
        second_flow,
        out_shape=[out],
        in_specs=vmem(6 + 9),
        out_specs=vmem(1),
        scratch_shapes=[buf] * 4,
        name="second_flow",
    )(
        *moving, end_places(2, ZR1, lambda i: (2 * i * ZR1, (2 * i + 1) * ZR1)), p1, s1,
        base, stress, biot, *links,
    )
    load = load_of(p2)
    disp = d_ext
    disp = mech(load, disp)
    strain = strain_of(disp)[..., :128]
    return (p2[ERIM : ERIM + cx, RIM : RIM + cy, :128], strain)


def solution(mesh):
    torus = Mesh(
        mesh.devices.reshape(mesh.shape["grp"], 4, 2, 2, mesh.shape["gy"]),
        ("grp", "gx_0", "gx_1", "gx_2", "gy"),
    )
    return jax.shard_map(
        per_device,
        mesh=torus,
        in_specs=(
            P(GX, "gy", "grp"),
            P(GX, "gy", "grp"),
            P(GX, "gy", "grp"),
            P(GX, "gy", "grp"),
            P(),
            P(),
            P(),
            P(GX, "gy", "grp", None, None),
            P(GX, "gy", "grp", None, None, None, None),
            P(GX, "gy", "grp"),
        ),
        out_specs=(P(GX, "gy", "grp"), P(GX, "gy", "grp")),
        check_vma=False,
    )
```

```python
import jax
import jax.numpy as jnp
import numpy as np
from jax import lax
from jax.experimental import pallas as pl
from jax.experimental.pallas import tpu as pltpu
from jax.sharding import Mesh
from jax.sharding import PartitionSpec as P

ITERS = 2
FLOW_PASSES = 4
MECH_PASSES = 3
OMEGA = 0.6
GX = ("gx_0", "gx_1", "gx_2")
BF = jnp.bfloat16
F32 = jnp.float32
RIM = 8
ZRIM = 14
ZR1 = 7
ERIM = 3


def row_order():
    order = np.zeros((32, 24), np.float32)
    sign = np.zeros((2, 2, 8), np.float32)
    for c in range(3):
        for dx in (0, 1):
            for dy in (0, 1):
                for dz in (0, 1):
                    order[8 * (2 * dx + dy) + 4 * dz + c, 8 * c + 4 * dx + 2 * dy + dz] = 1.0
                    sign[dx, dy, 4 * dz + c] = 0.25 * (2 * (dx, dy, dz)[c] - 1)
    return order, sign


def exchange(to_low, to_high, axis, periodic):
    count = lax.axis_size(axis)
    last = count if periodic else count - 1
    up = [(i, (i + 1) % count) for i in range(last)]
    down = [((i + 1) % count, i) for i in range(last)]
    return lax.ppermute(to_high, axis, up), lax.ppermute(to_low, axis, down)


def rows_of(*parts):
    return jnp.concatenate([p.reshape(-1, 128) for p in parts], axis=0)


def cut_rows(buffer, shapes):
    out, at = [], 0
    for shape in shapes:
        rows = int(np.prod(shape)) // 128
        out.append(buffer[at : at + rows].reshape(shape))
        at += rows
    return out


def lane_pad(a):
    return jnp.pad(a, [(0, 0)] * (a.ndim - 1) + [(0, 128 - a.shape[-1])])


def cut_along(array, dim, peers):
    lengths = array.shape
    parts = array.reshape(*lengths[:dim], peers, lengths[dim] // peers, *lengths[dim + 1 :])
    return jnp.moveaxis(parts, dim, 0)


def joined_along(parts, dim):
    lengths = list(parts.shape[1:])
    lengths[dim] *= parts.shape[0]
    return jnp.moveaxis(parts, 0, dim).reshape(lengths)


def exchange_in_order(parts, axes, order):
    lengths = [lax.axis_size(a) for a in axes]
    parts = parts.reshape(*lengths, *parts.shape[1:])
    for k in order:
        parts = lax.all_to_all(parts, axes[k], split_axis=k, concat_axis=k, tiled=True)
    return parts.reshape(-1, *parts.shape[len(axes) :])


def core_and_chips(array, groups, order, split_dim, concat_dim):
    peers = lax.axis_size(groups[0]) * lax.axis_size(groups[1])
    parts = cut_along(array, split_dim, peers)
    return joined_along(exchange_in_order(parts, groups, order), concat_dim)


def pick(rock, table):
    one_hot = (rock[None] == jnp.arange(table.shape[1], dtype=jnp.int32)[:, None, None, None]).astype(F32)
    return jnp.tensordot(table, one_hot, 1, precision=lax.Precision.HIGHEST)


def transmit(a, b):
    total = a + b
    return 2.0 * a * b / jnp.where(total > 0, total, 1.0)


def roll_up(a, axis):
    return pltpu.roll(a, a.shape[axis] - 1, axis)


def roll_down(a, axis):
    return pltpu.roll(a, 1, axis)


def flow_passes(start, spare, num, tx, ty, ty_low, tz, tz_low, inv_den, biot, load, out):
    ex = start.shape[0]
    cx, cy, width = out.shape
    for k in range(1, FLOW_PASSES + 1):
        src = start if k % 2 == 1 else spare
        dst = spare if k % 2 == 1 else start
        lo, hi = 1 + k, ex - 1 - k

        def step(x, carry):
            mid = src[x]
            total = (
                (num[x] + tx[x - 1] * src[x - 1])
                + (tx[x] * src[x + 1] + ty[x] * roll_up(mid, 0))
                + (ty_low[x] * roll_down(mid, 0) + tz[x] * roll_up(mid, 1))
                + tz_low[x] * roll_down(mid, 1)
            ) * inv_den[x]
            dst[x] = total
            if k == FLOW_PASSES:
                load[x - lo] = total * biot[x]
            return carry

        lax.fori_loop(lo, hi, step, 0, unroll=2)
    out[...] = start[RIM : RIM + cx, RIM : RIM + cy, :width]


def tile_row():
    return lax.broadcasted_iota(jnp.int32, (8, 256), 0)


def fold(g):
    swapped = pltpu.roll(g, 4, 0)
    return g + jnp.where(tile_row() < 4, roll_down(swapped, 1), roll_up(swapped, 1))


def brick_product(ko, ke, u_own, u_end):
    f_own = jnp.dot(ko, u_own, preferred_element_type=F32)
    f_end = jnp.dot(ke, u_end, preferred_element_type=F32)
    lane = lax.broadcasted_iota(jnp.int32, (32, 128), 1)
    f_end = jnp.where(lane < 64, f_end[:32], f_end[32:])
    return [jnp.concatenate([f_own[8 * q : 8 * q + 8], f_end[8 * q : 8 * q + 8]], axis=1) for q in range(4)]


def spread_rows(products, n, x, low_x, high_x):
    last = None
    for y in range(n):
        now = products(y)
        if last is not None:
            low_x[x, y - 1] = now[0] + last[1]
            high_x[x, y - 1] = now[2] + last[3]
        last = now


def elastic_static(held, k_own, k_ends, free, step, low_x, high_x):
    n = k_own.shape[0]
    eye = (lax.broadcasted_iota(jnp.int32, (64, 32), 0) % 32) == lax.broadcasted_iota(jnp.int32, (64, 32), 1)
    eye = jnp.where(eye, 1.0, 0.0)
    ones = jnp.ones((32, 128), BF)

    def bricks(x, carry):
        def product(y):
            ko = (k_own[x, y].astype(F32) * eye[:32]).astype(BF)
            ke = (k_ends[x, y].astype(F32) * eye).astype(BF)
            return brick_product(ko, ke, ones, ones)

        spread_rows(product, n, x, low_x, high_x)
        return carry

    lax.fori_loop(0, n, bricks, 0)

    def nodes(i, carry):
        m = RIM - ERIM
        for j in range(n - 1):
            diag = fold(low_x[i + 1, j] + high_x[i, j])
            near = [
                jnp.broadcast_to(held[i + m + a, j + m + b : j + m + b + 1, :], (8, 256))
                for a in (0, 1)
                for b in (0, 1)
            ]
            near = (near[0] + near[1]) + (near[2] + near[3])
            near = near + jnp.where(tile_row() < 4, roll_down(near, 1), roll_up(near, 1))
            loose = jnp.where(near > 0, 0.0, 1.0)
            free[i, j] = loose
            step[i, j] = jnp.where(diag > 0, OMEGA * loose / jnp.where(diag > 0, diag, 1.0), 0.0)
        return carry

    lax.fori_loop(0, n - 1, nodes, 0)


def elastic_load(bp, signs, load):
    n = bp.shape[0]
    m = RIM - ERIM

    def nodes(i, carry):
        sign = [signs[q] for q in range(4)]
        for j in range(n - 1):
            total = None
            for dx in (0, 1):
                for dy in (0, 1):
                    y = j + m + 1 - dy
                    term = jnp.broadcast_to(bp[i + 1 - dx, y : y + 1, :], (8, 256)) * sign[2 * dx + dy]
                    total = term if total is None else total + term
            load[i, j] = fold(total)
        return carry

    lax.fori_loop(0, n - 1, nodes, 0)


def elastic_pass(rim, disp, load, free, step, k_own, k_ends, low_x, high_x, cx):
    n, m = cx + 2 * rim, ERIM - rim

    def bricks(x, carry):
        def product(y):
            u = jnp.concatenate([disp[x + m + dx, y + m + dy] for dx in (0, 1) for dy in (0, 1)], axis=0).astype(BF)
            return brick_product(k_own[x + m, y + m], k_ends[x + m, y + m], u[:, :128], u[:, 128:])

        spread_rows(product, n, x, low_x, high_x)
        return carry

    lax.fori_loop(0, n, bricks, 0)

    def nodes(i, carry):
        for j in range(n - 1):
            residual = load[i + m, j + m] - fold(low_x[i + 1, j] + high_x[i, j])
            at = (i + m + 1, j + m + 1)
            disp[at] = free[i + m, j + m] * disp[at] + step[i + m, j + m] * residual
        return carry

    lax.fori_loop(0, n - 1, nodes, 0)


def elastic_strain(disp, signs, out):
    cx, cy, width = out.shape

    def cells(x, carry):
        sign = [signs[q] for q in range(4)]
        for y in range(cy):
            total = None
            for dx in (0, 1):
                for dy in (0, 1):
                    term = disp[x + ERIM + dx, y + ERIM + dy] * sign[2 * dx + dy]
                    total = term if total is None else total + term
            out[x, y : y + 1, :] = jnp.sum(total, axis=0, keepdims=True)[:, :width]
        return carry

    lax.fori_loop(0, cx, cells, 0)


def first_flow(
    table, z_range, fp, fc, fr, fh, ends, place, p_own, c_own, source, k_own, k_ends, signs,
    out, strain, packed, base, stress, biot, tx, ty, ty_low, tz, tz_low, inv_den, free, step,
    start, spare, cond, num, held, bp, disp, load, low_x, high_x,
):
    ex, ey = start.shape[0], start.shape[1]
    cx = p_own.shape[0]
    lane = lax.broadcasted_iota(jnp.int32, (ey, 256), 1)
    z_at = jnp.where(lane < 192, lane, lane - 256) + z_range[0]
    z_in = (z_at >= 0) & (z_at < z_range[1])

    def choose(rock, row):
        value = jnp.full(rock.shape, table[row, 3], F32)
        for r in range(3):
            value = jnp.where(rock == float(r), table[row, r], value)
        return value

    def gather(x, carry):
        apart = jnp.dot(ends[x], place[...], preferred_element_type=F32)
        start[x] = jnp.concatenate([fp[x].astype(F32), apart[:, :128]], axis=1)
        cond[x] = jnp.concatenate([fc[x].astype(F32), apart[:, 128:256]], axis=1)
        rock = jnp.concatenate([fr[x].astype(F32), apart[:, 256:384]], axis=1)
        held[x] = jnp.concatenate([fh[x].astype(F32), apart[:, 384:]], axis=1)
        storage = choose(rock, 2)
        strained = choose(rock, 3)
        base[x] = storage
        stress[x] = strained
        biot[x] = jnp.where(z_in, choose(rock, 4), 0.0)
        inv_den[x] = storage + strained
        return carry

    lax.fori_loop(0, ex, gather, 0, unroll=2)
    start[RIM : RIM + cx, RIM : RIM + p_own.shape[1], 0:128] = p_own[...]
    cond[RIM : RIM + cx, RIM : RIM + p_own.shape[1], 0:128] = c_own[...]

    def static_terms(x, carry):
        c = cond[x]
        tx[x] = transmit(c, cond[jnp.minimum(x + 1, ex - 1)])
        t = transmit(c, roll_up(c, 0))
        low = roll_down(t, 0)
        ty[x] = t
        ty_low[x] = low
        den = inv_den[x] + t + low
        t = transmit(c, roll_up(c, 1))
        low = roll_down(t, 1)
        tz[x] = t
        tz_low[x] = low
        p = start[x]
        b = base[x] * p + source[x]
        base[x] = b
        num[x] = b + stress[x] * p
        inv_den[x] = 1.0 / (den + t + low + tx[x] + tx[jnp.maximum(x - 1, 0)])
        return carry

    lax.fori_loop(0, ex, static_terms, 0, unroll=2)
    flow_passes(start, spare, num, tx, ty, ty_low, tz, tz_low, inv_den, biot, bp, out)
    elastic_static(held, k_own, k_ends, free, step, low_x, high_x)
    elastic_load(bp, signs, load)

    def first_pass(i, carry):
        for j in range(free.shape[1]):
            disp[i + 1, j + 1] = step[i, j] * load[i, j]
        return carry

    lax.fori_loop(0, free.shape[0], first_pass, 0)
    for k in range(1, MECH_PASSES):
        elastic_pass(ERIM - k, disp, load, free, step, k_own, k_ends, low_x, high_x, cx)
    elastic_strain(disp, signs, strain)

    def pack(i, carry):
        for j in range(packed.shape[1]):
            d = disp[i + ERIM, j + ERIM]
            packed[i, j] = jnp.where(tile_row()[:, :128] < 4, d[:, :128], pltpu.roll(d[:, 128:], 4, 0))
        return carry

    lax.fori_loop(0, packed.shape[0], pack, 0)


def second_flow(
    fp, fs, ends, place, p_own, s_own, d_ext, d_own, k_own, k_ends, signs,
    base, stress, biot, tx, ty, ty_low, tz, tz_low, inv_den, free, step,
    out, strain_out, start, spare, num, strain, bp, disp, load, low_x, high_x,
):
    ex = start.shape[0]
    cx, cy = p_own.shape[0], p_own.shape[1]

    def gather(x, carry):
        apart = jnp.dot(ends[x], place[...], preferred_element_type=F32)
        start[x] = jnp.concatenate([fp[x].astype(F32), apart[:, :128]], axis=1)
        strain[x] = jnp.concatenate([fs[x].astype(F32), apart[:, 128:]], axis=1)
        return carry

    lax.fori_loop(0, ex, gather, 0, unroll=2)
    start[RIM : RIM + cx, RIM : RIM + cy, :] = p_own[...]
    strain[RIM : RIM + cx, RIM : RIM + cy, :] = s_own[...]

    def numerator(x, carry):
        num[x] = base[x] + stress[x] * start[x] - biot[x] * strain[x]
        return carry

    lax.fori_loop(2, ex - 2, numerator, 0, unroll=2)
    flow_passes(start, spare, num, tx, ty, ty_low, tz, tz_low, inv_den, biot, bp, out)
    elastic_load(bp, signs, load)

    def unpacked(d):
        wide = jnp.concatenate([d, pltpu.roll(d, 4, 0)], axis=1)
        return jnp.where(tile_row() < 4, wide, pltpu.roll(roll_up(wide, 1), 4, 0))

    def unpack(i, carry):
        for j in range(d_ext.shape[1]):
            disp[i, j] = unpacked(d_ext[i, j].astype(F32))
        return carry

    lax.fori_loop(0, d_ext.shape[0], unpack, 0)

    def unpack_own(i, carry):
        for j in range(d_own.shape[1]):
            disp[i + ERIM, j + ERIM] = unpacked(d_own[i, j])
        return carry

    lax.fori_loop(0, d_own.shape[0], unpack_own, 0)
    for k in range(MECH_PASSES):
        elastic_pass(ERIM - k, disp, load, free, step, k_own, k_ends, low_x, high_x, cx)
    elastic_strain(disp, signs, strain_out)


def vmem(n):
    return [pl.BlockSpec(memory_space=pltpu.VMEM)] * n


def end_places(count, width, fields):
    place = np.zeros((128, 128 * count), np.float32)
    for i in range(count):
        after, ahead = fields(i)
        for t in range(width):
            place[after + t, 128 * i + t] = 1.0
            place[ahead + t, 128 * i + 128 - width + t] = 1.0
    return jnp.asarray(place, BF)


def per_device(
    pressure_start,
    saturation,
    permeability,
    rock_type,
    rock_table,
    well_cells,
    well_rates,
    owner_map,
    stiffness,
    anchored,
):
    cx, cy, cz = pressure_start.shape
    count_x = lax.axis_size(GX)
    total_x = cx * count_x
    total_y = cy * lax.axis_size("gy")
    total_z = cz * lax.axis_size("grp")
    start_x = lax.axis_index(GX) * cx
    start_y = lax.axis_index("gy") * cy
    start_z = lax.axis_index("grp") * cz
    order, sign = row_order()
    ex, ey = cx + 2 * RIM, cy + 2 * RIM

    owners = owner_map.reshape(-1)
    capacity = stiffness.shape[4]
    one_hot = (owners[:, None] == jnp.arange(count_x, dtype=jnp.int32)[None, :]).astype(jnp.int32)
    before = jnp.cumsum(one_hot, axis=0) - one_hot
    brick_rank = jnp.sum(before * one_hot, axis=1)
    lanes_of = np.zeros((4, 24, 128), np.float32)
    for j in range(4):
        lanes_of[j, :, 32 * j : 32 * j + 32] = order.T
    lanes_of = jnp.asarray(lanes_of, BF)
    held_blocks = stiffness.reshape(count_x, capacity // 4, 4, 24, 24)
    packed = sum(
        jnp.einsum("ogrk,km->ogrm", held_blocks[:, :, j], lanes_of[j], preferred_element_type=F32) for j in range(4)
    ).astype(BF)
    fetched = core_and_chips(packed, (("gx_0", "gx_1"), "gx_2"), (1, 0), 0, 0)
    groups = fetched.reshape(count_x * (capacity // 4), 24, 128)[owners * (capacity // 4) + brick_rank // 4]
    lane_at = lax.broadcasted_iota(jnp.int32, groups.shape, 2) // 32
    groups = jnp.where(lane_at == (brick_rank % 4)[:, None, None], groups, 0)
    fold = jnp.asarray(np.tile(np.eye(32, dtype=np.float32), (4, 1)), BF)
    half = jnp.einsum("brm,mc->brc", groups, fold, preferred_element_type=F32).astype(BF)
    block = jnp.einsum("ar,brc->bac", jnp.asarray(order, BF), half, preferred_element_type=F32).astype(BF)
    block = block.reshape(cx, cy, 32, 32)

    exponents = pick(rock_type, rock_table[:2])
    mobility = jnp.exp(exponents[0] * jnp.log(saturation)) + 2.0 * jnp.exp(
        exponents[1] * jnp.log(1.0 - saturation)
    )
    conductance = permeability * mobility
    fields = [a.astype(BF) for a in (pressure_start, conductance, rock_type, anchored)]

    def k_lanes(b):
        return lane_pad(jnp.concatenate([b[:, i] for i in range(ERIM)], axis=-1))

    got = exchange(
        rows_of(*fields, k_lanes(block[:, :ERIM])),
        rows_of(*fields, k_lanes(block[:, cy - ERIM :])),
        "gy",
        False,
    )
    shapes = [(cx, cy, cz)] * 4 + [(cx, 32, 128)]
    low, high = cut_rows(got[0], shapes), cut_rows(got[1], shapes)
    fields = [jnp.concatenate([low[i], fields[i], high[i]], axis=1) for i in range(4)]

    def k_apart(lanes):
        return jnp.stack([lanes[:, :, 32 * i : 32 * i + 32] for i in range(ERIM)], axis=1)

    block = jnp.concatenate([k_apart(low[4]), block, k_apart(high[4])], axis=1)
    ky = cy + 2 * ERIM

    quad = block.reshape(2, 4, ky, 32, 32)
    quad = jnp.concatenate([quad[:, i] for i in range(4)], axis=-1)
    got = exchange(
        rows_of(lane_pad(jnp.concatenate([f[..., :ZRIM] for f in fields], axis=-1)), quad),
        rows_of(lane_pad(jnp.concatenate([f[..., cz - ZRIM :] for f in fields], axis=-1)), quad),
        "grp",
        False,
    )
    shapes = [(cx, ey, 128), (2, ky, 32, 128)]
    low, high = cut_rows(got[0], shapes), cut_rows(got[1], shapes)
    ends = lane_pad(jnp.concatenate([high[0][..., : 4 * ZRIM], low[0][..., : 4 * ZRIM]], axis=-1))

    def quad_apart(q):
        return jnp.stack([q[..., 32 * i : 32 * i + 32] for i in range(4)], axis=1).reshape(cx, ky, 32, 32)

    after, ahead = quad_apart(high[1]), quad_apart(low[1])

    def k_three(cut):
        return lane_pad(jnp.concatenate([block[cut], after[cut], ahead[cut]], axis=-1))

    got = exchange(
        rows_of(*fields, ends, k_three(slice(0, ERIM))),
        rows_of(*fields, ends, k_three(slice(cx - ERIM, cx))),
        GX,
        True,
    )
    shapes = [(cx, ey, 128)] * 5 + [(ERIM, ky, 32, 128)]
    low, high = cut_rows(got[0], shapes), cut_rows(got[1], shapes)
    fields = [jnp.concatenate([low[i], fields[i], high[i]], axis=0) for i in range(4)]
    ends = jnp.concatenate([low[4], ends, high[4]], axis=0)
    k_own = jnp.concatenate([low[5][..., :32], block, high[5][..., :32]], axis=0)
    k_ends = jnp.concatenate(
        [
            jnp.concatenate([low[5][..., 32:64], after, high[5][..., 32:64]], axis=0),
            jnp.concatenate([low[5][..., 64:96], ahead, high[5][..., 64:96]], axis=0),
        ],
        axis=2,
    )

    plane = total_y * total_z
    well_x = (well_cells // plane - start_x + RIM) % total_x
    well_y = well_cells // total_z % total_y - start_y + RIM
    well_z = well_cells % total_z - start_z
    near = (well_z >= -ZRIM) & (well_z < cz + ZRIM)
    lane = jnp.where(near, well_z % 256, -1)
    at_x = (jnp.arange(ex, dtype=jnp.int32)[:, None] == well_x[None, :]).astype(F32)
    at_y = (jnp.arange(ey, dtype=jnp.int32)[:, None] == well_y[None, :]).astype(F32)
    at_xy = (at_x[:, None, :] * at_y[None, :, :]).reshape(ex * ey, -1)
    at_z = jnp.where(lane[:, None] == jnp.arange(256, dtype=jnp.int32)[None, :], well_rates[:, None], 0.0)
    source = jnp.dot(at_xy, at_z, precision=lax.Precision.HIGHEST).reshape(ex, ey, 256)
    cells = jax.ShapeDtypeStruct((ex, ey, 256), F32)
    tall = jax.ShapeDtypeStruct((cx, cy, 256), F32)
    n = cx + 2 * ERIM
    node = jax.ShapeDtypeStruct((n - 1, n - 1, 8, 256), F32)
    buf = pltpu.VMEM((ex, ey, 256), F32)
    bp_buf = pltpu.VMEM((n, ey, 256), F32)
    elastic_bufs = [
        pltpu.VMEM((n + 1, n + 1, 8, 256), F32),
        pltpu.VMEM((n - 1, n - 1, 8, 256), F32),
        pltpu.VMEM((n, n - 1, 8, 256), F32),
        pltpu.VMEM((n, n - 1, 8, 256), F32),
    ]
    signs = jnp.asarray(np.broadcast_to(sign.reshape(4, 8, 1), (4, 8, 256)), F32)
    z_range = jnp.stack([start_z, jnp.int32(total_z)]).astype(jnp.int32)
    p1, s1, d_pack, *static = pl.pallas_call(
        first_flow,
        out_shape=[tall, tall, jax.ShapeDtypeStruct((cx + 1, cy + 1, 8, 128), F32)] + [cells] * 9 + [node] * 2,
        in_specs=[pl.BlockSpec(memory_space=pltpu.SMEM)] * 2 + vmem(12),
        out_specs=vmem(14),
        scratch_shapes=[buf] * 5 + [bp_buf] + elastic_bufs,
        name="first_iteration",
    )(
        rock_table, z_range, *fields, ends, end_places(4, ZRIM, lambda i: (i * ZRIM, (4 + i) * ZRIM)),
        pressure_start, conductance, source, k_own, k_ends, signs,
    )

    def ends_of(a):
        return jnp.concatenate([a[..., 128 : 128 + ZR1], a[..., 256 - ZR1 :]], axis=-1)

    p_bf, s_bf = p1.astype(BF), s1.astype(BF)
    moving = [p_bf[..., :128], s_bf[..., :128], lane_pad(jnp.concatenate([ends_of(p_bf), ends_of(s_bf)], axis=-1))]
    d_bf = d_pack.astype(BF)
    got = exchange(
        rows_of(*moving, d_bf[:, 1 : 1 + ERIM]),
        rows_of(*moving, d_bf[:, cy - ERIM : cy]),
        "gy",
        False,
    )
    shapes = [(cx, cy, 128)] * 3 + [(cx + 1, ERIM, 8, 128)]
    low, high = cut_rows(got[0], shapes), cut_rows(got[1], shapes)
    moving = [jnp.concatenate([low[i], moving[i], high[i]], axis=1) for i in range(3)]
    d_bf = jnp.concatenate([low[3], d_bf, high[3]], axis=1)
    got = exchange(
        rows_of(*moving, d_bf[1 : 1 + ERIM]),
        rows_of(*moving, d_bf[cx - ERIM : cx]),
        GX,
        True,
    )
    shapes = [(cx, ey, 128)] * 3 + [(ERIM, cy + 1 + 2 * ERIM, 8, 128)]
    low, high = cut_rows(got[0], shapes), cut_rows(got[1], shapes)
    moving = [jnp.concatenate([low[i], moving[i], high[i]], axis=0) for i in range(3)]
    d_bf = jnp.concatenate([low[3], d_bf, high[3]], axis=0)
    short = jax.ShapeDtypeStruct((cx, cy, cz), F32)
    return pl.pallas_call(
        second_flow,
        out_shape=[short, short],
        in_specs=vmem(11 + 11),
        out_specs=vmem(2),
        scratch_shapes=[buf] * 4 + [bp_buf] + elastic_bufs,
        name="second_iteration",
    )(
        *moving, end_places(2, ZR1, lambda i: (2 * i * ZR1, (2 * i + 1) * ZR1)), p1, s1,
        d_bf, d_pack, k_own, k_ends, signs, *static,
    )


def solution(mesh):
    torus = Mesh(
        mesh.devices.reshape(mesh.shape["grp"], 4, 2, 2, mesh.shape["gy"]),
        ("grp", "gx_0", "gx_1", "gx_2", "gy"),
    )
    return jax.shard_map(
        per_device,
        mesh=torus,
        in_specs=(
            P(GX, "gy", "grp"),
            P(GX, "gy", "grp"),
            P(GX, "gy", "grp"),
            P(GX, "gy", "grp"),
            P(),
            P(),
            P(),
            P(GX, "gy", "grp", None, None),
            P(GX, "gy", "grp", None, None, None, None),
            P(GX, "gy", "grp"),
        ),
        out_specs=(P(GX, "gy", "grp"), P(GX, "gy", "grp")),
        check_vma=False,
    )
```

```python
import jax
import jax.numpy as jnp
import numpy as np
from jax import lax
from jax.experimental import pallas as pl
from jax.experimental.pallas import tpu as pltpu
from jax.sharding import Mesh
from jax.sharding import PartitionSpec as P

ITERS = 2
FLOW_PASSES = 4
MECH_PASSES = 3
OMEGA = 0.6
GX = ("gx_0", "gx_1", "gx_2")
BF = jnp.bfloat16
F32 = jnp.float32
RIM = 8
ZRIM = (13, 13, 13, 13, 10)
ZSIDE = sum(ZRIM)
ZR1 = 7
ERIM = 3


def row_order():
    order = np.zeros((32, 24), np.float32)
    sign = np.zeros((2, 2, 8), np.float32)
    for c in range(3):
        for dx in (0, 1):
            for dy in (0, 1):
                for dz in (0, 1):
                    order[8 * (2 * dx + dy) + 4 * dz + c, 8 * c + 4 * dx + 2 * dy + dz] = 1.0
                    sign[dx, dy, 4 * dz + c] = 0.25 * (2 * (dx, dy, dz)[c] - 1)
    return order, sign


def exchange(to_low, to_high, axis, periodic):
    count = lax.axis_size(axis)
    last = count if periodic else count - 1
    up = [(i, (i + 1) % count) for i in range(last)]
    down = [((i + 1) % count, i) for i in range(last)]
    return lax.ppermute(to_high, axis, up), lax.ppermute(to_low, axis, down)


def rows_of(*parts):
    return jnp.concatenate([p.reshape(-1, 128) for p in parts], axis=0)


def cut_rows(buffer, shapes):
    out, at = [], 0
    for shape in shapes:
        rows = int(np.prod(shape)) // 128
        out.append(buffer[at : at + rows].reshape(shape))
        at += rows
    return out


def lane_pad(a):
    return jnp.pad(a, [(0, 0)] * (a.ndim - 1) + [(0, 128 - a.shape[-1])])


def cut_along(array, dim, peers):
    lengths = array.shape
    parts = array.reshape(*lengths[:dim], peers, lengths[dim] // peers, *lengths[dim + 1 :])
    return jnp.moveaxis(parts, dim, 0)


def joined_along(parts, dim):
    lengths = list(parts.shape[1:])
    lengths[dim] *= parts.shape[0]
    return jnp.moveaxis(parts, 0, dim).reshape(lengths)


def exchange_in_order(parts, axes, order):
    lengths = [lax.axis_size(a) for a in axes]
    parts = parts.reshape(*lengths, *parts.shape[1:])
    for k in order:
        parts = lax.all_to_all(parts, axes[k], split_axis=k, concat_axis=k, tiled=True)
    return parts.reshape(-1, *parts.shape[len(axes) :])


def core_and_chips(array, groups, order, split_dim, concat_dim):
    peers = lax.axis_size(groups[0]) * lax.axis_size(groups[1])
    parts = cut_along(array, split_dim, peers)
    return joined_along(exchange_in_order(parts, groups, order), concat_dim)


def pick(rock, table):
    one_hot = (rock[None] == jnp.arange(table.shape[1], dtype=jnp.int32)[:, None, None, None]).astype(F32)
    return jnp.tensordot(table, one_hot, 1, precision=lax.Precision.HIGHEST)


def transmit(a, b):
    total = a + b
    return 2.0 * a * b / jnp.where(total > 0, total, 1.0)


def roll_up(a, axis):
    return pltpu.roll(a, a.shape[axis] - 1, axis)


def roll_down(a, axis):
    return pltpu.roll(a, 1, axis)


def flow_passes(start, spare, num, tx, ty, ty_low, tz, tz_low, inv_den, biot, load, out):
    ex = start.shape[0]
    cx, cy, width = out.shape
    for k in range(1, FLOW_PASSES + 1):
        src = start if k % 2 == 1 else spare
        dst = spare if k % 2 == 1 else start
        lo, hi = 1 + k, ex - 1 - k

        def step(x, carry):
            mid = src[x]
            total = (
                (num[x] + tx[x - 1] * src[x - 1])
                + (tx[x] * src[x + 1] + ty[x] * roll_up(mid, 0))
                + (ty_low[x] * roll_down(mid, 0) + tz[x] * roll_up(mid, 1))
                + tz_low[x] * roll_down(mid, 1)
            ) * inv_den[x]
            dst[x] = total
            if k == FLOW_PASSES:
                load[x - lo] = total * biot[x]
            return carry

        lax.fori_loop(lo, hi, step, 0, unroll=2)
    out[...] = start[RIM : RIM + cx, RIM : RIM + cy, :width]


def tile_row():
    return lax.broadcasted_iota(jnp.int32, (8, 256), 0)


def fold(g):
    swapped = pltpu.roll(g, 4, 0)
    return g + jnp.where(tile_row() < 4, roll_down(swapped, 1), roll_up(swapped, 1))


def brick_product(ko, ke, u_own, u_end):
    f_own = jnp.dot(ko, u_own, preferred_element_type=F32)
    f_end = jnp.dot(ke, u_end, preferred_element_type=F32)
    lane = lax.broadcasted_iota(jnp.int32, (32, 128), 1)
    f_end = jnp.where(lane < 64, f_end[:32], f_end[32:])
    return [jnp.concatenate([f_own[8 * q : 8 * q + 8], f_end[8 * q : 8 * q + 8]], axis=1) for q in range(4)]


def spread_rows(products, n, x, low_x, high_x):
    last = None
    for y in range(n):
        now = products(y)
        if last is not None:
            low_x[x, y - 1] = now[0] + last[1]
            high_x[x, y - 1] = now[2] + last[3]
        last = now


def elastic_static(held, k_own, k_ends, free, step, low_x, high_x):
    n = k_own.shape[0]
    eye = (lax.broadcasted_iota(jnp.int32, (64, 32), 0) % 32) == lax.broadcasted_iota(jnp.int32, (64, 32), 1)
    eye = jnp.where(eye, 1.0, 0.0)
    ones = jnp.ones((32, 128), BF)

    def bricks(x, carry):
        def product(y):
            ko = (k_own[x, y].astype(F32) * eye[:32]).astype(BF)
            ke = (k_ends[x, y].astype(F32) * eye).astype(BF)
            return brick_product(ko, ke, ones, ones)

        spread_rows(product, n, x, low_x, high_x)
        return carry

    lax.fori_loop(0, n, bricks, 0)

    def nodes(i, carry):
        m = RIM - ERIM
        for j in range(n - 1):
            diag = fold(low_x[i + 1, j] + high_x[i, j])
            near = [
                jnp.broadcast_to(held[i + m + a, j + m + b : j + m + b + 1, :], (8, 256))
                for a in (0, 1)
                for b in (0, 1)
            ]
            near = (near[0] + near[1]) + (near[2] + near[3])
            near = near + jnp.where(tile_row() < 4, roll_down(near, 1), roll_up(near, 1))
            loose = jnp.where(near > 0, 0.0, 1.0)
            free[i, j] = loose
            step[i, j] = jnp.where(diag > 0, OMEGA * loose / jnp.where(diag > 0, diag, 1.0), 0.0)
        return carry

    lax.fori_loop(0, n - 1, nodes, 0)


def elastic_load(bp, signs, load):
    n = bp.shape[0]
    m = RIM - ERIM

    def nodes(i, carry):
        sign = [signs[q] for q in range(4)]
        for j in range(n - 1):
            total = None
            for dx in (0, 1):
                for dy in (0, 1):
                    y = j + m + 1 - dy
                    term = jnp.broadcast_to(bp[i + 1 - dx, y : y + 1, :], (8, 256)) * sign[2 * dx + dy]
                    total = term if total is None else total + term
            load[i, j] = fold(total)
        return carry

    lax.fori_loop(0, n - 1, nodes, 0)


def elastic_pass(rim, disp, load, free, step, k_own, k_ends, low_x, high_x, cx):
    n, m = cx + 2 * rim, ERIM - rim

    def bricks(x, carry):
        def product(y):
            u = jnp.concatenate([disp[x + m + dx, y + m + dy] for dx in (0, 1) for dy in (0, 1)], axis=0).astype(BF)
            return brick_product(k_own[x + m, y + m], k_ends[x + m, y + m], u[:, :128], u[:, 128:])

        spread_rows(product, n, x, low_x, high_x)
        return carry

    lax.fori_loop(0, n, bricks, 0)

    def nodes(i, carry):
        for j in range(n - 1):
            residual = load[i + m, j + m] - fold(low_x[i + 1, j] + high_x[i, j])
            at = (i + m + 1, j + m + 1)
            disp[at] = free[i + m, j + m] * disp[at] + step[i + m, j + m] * residual
        return carry

    lax.fori_loop(0, n - 1, nodes, 0)


def elastic_strain(disp, signs, out):
    cx, cy, width = out.shape

    def cells(x, carry):
        sign = [signs[q] for q in range(4)]
        for y in range(cy):
            total = None
            for dx in (0, 1):
                for dy in (0, 1):
                    term = disp[x + ERIM + dx, y + ERIM + dy] * sign[2 * dx + dy]
                    total = term if total is None else total + term
            out[x, y : y + 1, :] = jnp.sum(total, axis=0, keepdims=True)[:, :width]
        return carry

    lax.fori_loop(0, cx, cells, 0)


def first_flow(
    table, z_range, below, above, f0, f1, f2, f3, f4, ends, place, p_own, c_own, source, k_own, k_ends, signs,
    out, strain, packed, base, stress, biot, tx, ty, ty_low, tz, tz_low, inv_den, free, step,
    start, spare, cond, num, held, bp, disp, load, low_x, high_x,
):
    ex, ey = start.shape[0], start.shape[1]
    cx = p_own.shape[0]
    lane = lax.broadcasted_iota(jnp.int32, (ey, 256), 1)
    z_at = jnp.where(lane < 192, lane, lane - 256) + z_range[0]
    z_in = (z_at >= 0) & (z_at < z_range[1])

    def choose(rock, row):
        value = jnp.full(rock.shape, table[row, 3], F32)
        for r in range(3):
            value = jnp.where(rock == float(r), table[row, r], value)
        return value

    def gather(plane, offset):
        def one(i, carry):
            x = i + offset
            apart = jnp.dot(plane(5, i), place[...], preferred_element_type=F32)
            fine = plane(0, i).astype(F32) + plane(1, i).astype(F32)
            start[x] = jnp.concatenate([fine, apart[:, :128]], axis=1)
            cond[x] = jnp.concatenate([plane(2, i).astype(F32), apart[:, 128:256]], axis=1)
            rock = jnp.concatenate([plane(3, i).astype(F32), apart[:, 256:384]], axis=1)
            held[x] = jnp.concatenate([plane(4, i).astype(F32), apart[:, 384:]], axis=1)
            storage = choose(rock, 2)
            strained = choose(rock, 3)
            base[x] = storage
            stress[x] = strained
            biot[x] = jnp.where(z_in, choose(rock, 4), 0.0)
            inv_den[x] = storage + strained
            return carry

        lax.fori_loop(0, RIM, one, 0, unroll=2)

    own = (f0, f1, f2, f3, f4, ends)
    gather(lambda f, i: below[f * RIM + i], 0)
    gather(lambda f, i: own[f][i], RIM)
    gather(lambda f, i: above[f * RIM + i], RIM + cx)
    start[RIM : RIM + cx, RIM : RIM + p_own.shape[1], 0:128] = p_own[...]
    cond[RIM : RIM + cx, RIM : RIM + p_own.shape[1], 0:128] = c_own[...]

    def static_terms(x, carry):
        c = cond[x]
        tx[x] = transmit(c, cond[jnp.minimum(x + 1, ex - 1)])
        t = transmit(c, roll_up(c, 0))
        low = roll_down(t, 0)
        ty[x] = t
        ty_low[x] = low
        den = inv_den[x] + t + low
        t = transmit(c, roll_up(c, 1))
        low = roll_down(t, 1)
        tz[x] = t
        tz_low[x] = low
        p = start[x]
        b = base[x] * p + source[x]
        base[x] = b
        num[x] = b + stress[x] * p
        inv_den[x] = 1.0 / (den + t + low + tx[x] + tx[jnp.maximum(x - 1, 0)])
        return carry

    lax.fori_loop(0, ex, static_terms, 0, unroll=2)
    flow_passes(start, spare, num, tx, ty, ty_low, tz, tz_low, inv_den, biot, bp, out)
    elastic_static(held, k_own, k_ends, free, step, low_x, high_x)
    elastic_load(bp, signs, load)

    def first_pass(i, carry):
        for j in range(free.shape[1]):
            disp[i + 1, j + 1] = step[i, j] * load[i, j]
        return carry

    lax.fori_loop(0, free.shape[0], first_pass, 0)
    for k in range(1, MECH_PASSES):
        elastic_pass(ERIM - k, disp, load, free, step, k_own, k_ends, low_x, high_x, cx)
    elastic_strain(disp, signs, strain)

    def pack(i, carry):
        for j in range(packed.shape[1]):
            d = disp[i + ERIM, j + ERIM]
            packed[i, j] = jnp.where(tile_row()[:, :128] < 4, d[:, :128], pltpu.roll(d[:, 128:], 4, 0))
        return carry

    lax.fori_loop(0, packed.shape[0], pack, 0)


def second_flow(
    below, above, f0, f1, f2, ends, place, p_own, s_own, d_ext, d_own, k_own, k_ends, signs,
    base, stress, biot, tx, ty, ty_low, tz, tz_low, inv_den, free, step,
    out, strain_out, start, spare, num, strain, bp, disp, load, low_x, high_x,
):
    ex = start.shape[0]
    cx, cy = p_own.shape[0], p_own.shape[1]

    def gather(plane, offset):
        def one(i, carry):
            x = i + offset
            apart = jnp.dot(plane(3, i), place[...], preferred_element_type=F32)
            fine = plane(0, i).astype(F32) + plane(1, i).astype(F32)
            start[x] = jnp.concatenate([fine, apart[:, :128]], axis=1)
            strain[x] = jnp.concatenate([plane(2, i).astype(F32), apart[:, 128:]], axis=1)
            return carry

        lax.fori_loop(0, RIM, one, 0, unroll=2)

    own = (f0, f1, f2, ends)
    gather(lambda f, i: below[f * RIM + i], 0)
    gather(lambda f, i: own[f][i], RIM)
    gather(lambda f, i: above[f * RIM + i], RIM + cx)
    start[RIM : RIM + cx, RIM : RIM + cy, :] = p_own[...]
    strain[RIM : RIM + cx, RIM : RIM + cy, :] = s_own[...]

    def numerator(x, carry):
        num[x] = base[x] + stress[x] * start[x] - biot[x] * strain[x]
        return carry

    lax.fori_loop(2, ex - 2, numerator, 0, unroll=2)
    flow_passes(start, spare, num, tx, ty, ty_low, tz, tz_low, inv_den, biot, bp, out)
    elastic_load(bp, signs, load)

    def unpacked(d):
        wide = jnp.concatenate([d, pltpu.roll(d, 4, 0)], axis=1)
        return jnp.where(tile_row() < 4, wide, pltpu.roll(roll_up(wide, 1), 4, 0))

    def unpack(i, carry):
        for j in range(d_ext.shape[1]):
            disp[i, j] = unpacked(d_ext[i, j].astype(F32))
        return carry

    lax.fori_loop(0, d_ext.shape[0], unpack, 0)

    def unpack_own(i, carry):
        for j in range(d_own.shape[1]):
            disp[i + ERIM, j + ERIM] = unpacked(d_own[i, j])
        return carry

    lax.fori_loop(0, d_own.shape[0], unpack_own, 0)
    for k in range(MECH_PASSES):
        elastic_pass(ERIM - k, disp, load, free, step, k_own, k_ends, low_x, high_x, cx)
    elastic_strain(disp, signs, strain_out)


def vmem(n):
    return [pl.BlockSpec(memory_space=pltpu.VMEM)] * n


def end_places(pieces):
    place = np.zeros((128, 128 * (1 + max(p[0] for p in pieces))), np.float32)
    for tile, width, after, ahead in pieces:
        for t in range(width):
            place[after + t, 128 * tile + t] = 1.0
            place[ahead + t, 128 * tile + 128 - width + t] = 1.0
    return jnp.asarray(place, BF)


def halves(a):
    high = lax.reduce_precision(a, 8, 7)
    return high.astype(BF), (a - high).astype(BF)


def per_device(
    pressure_start,
    saturation,
    permeability,
    rock_type,
    rock_table,
    well_cells,
    well_rates,
    owner_map,
    stiffness,
    anchored,
):
    cx, cy, cz = pressure_start.shape
    count_x = lax.axis_size(GX)
    total_x = cx * count_x
    total_y = cy * lax.axis_size("gy")
    total_z = cz * lax.axis_size("grp")
    start_x = lax.axis_index(GX) * cx
    start_y = lax.axis_index("gy") * cy
    start_z = lax.axis_index("grp") * cz
    order, sign = row_order()
    ex, ey = cx + 2 * RIM, cy + 2 * RIM

    owners = owner_map.reshape(-1)
    capacity = stiffness.shape[4]
    one_hot = (owners[:, None] == jnp.arange(count_x, dtype=jnp.int32)[None, :]).astype(jnp.int32)
    before = jnp.cumsum(one_hot, axis=0) - one_hot
    brick_rank = jnp.sum(before * one_hot, axis=1)
    lanes_of = np.zeros((4, 24, 128), np.float32)
    for j in range(4):
        lanes_of[j, :, 32 * j : 32 * j + 32] = order.T
    lanes_of = jnp.asarray(lanes_of, BF)
    held_blocks = stiffness.reshape(count_x, capacity // 4, 4, 24, 24)
    packed = sum(
        jnp.einsum("ogrk,km->ogrm", held_blocks[:, :, j], lanes_of[j], preferred_element_type=F32) for j in range(4)
    ).astype(BF)
    fetched = core_and_chips(packed, (("gx_0", "gx_1"), "gx_2"), (1, 0), 0, 0)
    groups = fetched.reshape(count_x * (capacity // 4), 24, 128)[owners * (capacity // 4) + brick_rank // 4]
    lane_at = lax.broadcasted_iota(jnp.int32, groups.shape, 2) // 32
    groups = jnp.where(lane_at == (brick_rank % 4)[:, None, None], groups, 0)
    fold = jnp.asarray(np.tile(np.eye(32, dtype=np.float32), (4, 1)), BF)
    half = jnp.einsum("brm,mc->brc", groups, fold, preferred_element_type=F32).astype(BF)
    block = jnp.einsum("ar,brc->bac", jnp.asarray(order, BF), half, preferred_element_type=F32).astype(BF)
    block = block.reshape(cx, cy, 32, 32)

    exponents = pick(rock_type, rock_table[:2])
    mobility = jnp.exp(exponents[0] * jnp.log(saturation)) + 2.0 * jnp.exp(
        exponents[1] * jnp.log(1.0 - saturation)
    )
    conductance = permeability * mobility
    fields = [*halves(pressure_start)] + [a.astype(BF) for a in (conductance, rock_type, anchored)]

    def k_lanes(b):
        return lane_pad(jnp.concatenate([b[:, i] for i in range(ERIM)], axis=-1))

    got = exchange(
        rows_of(*fields, k_lanes(block[:, :ERIM])),
        rows_of(*fields, k_lanes(block[:, cy - ERIM :])),
        "gy",
        False,
    )
    shapes = [(cx, cy, cz)] * 5 + [(cx, 32, 128)]
    low, high = cut_rows(got[0], shapes), cut_rows(got[1], shapes)
    fields = [jnp.concatenate([low[i], fields[i], high[i]], axis=1) for i in range(5)]

    def k_apart(lanes):
        return jnp.stack([lanes[:, :, 32 * i : 32 * i + 32] for i in range(ERIM)], axis=1)

    block = jnp.concatenate([k_apart(low[5]), block, k_apart(high[5])], axis=1)
    ky = cy + 2 * ERIM

    quad = block.reshape(2, 4, ky, 32, 32)
    quad = jnp.concatenate([quad[:, i] for i in range(4)], axis=-1)
    got = exchange(
        rows_of(lane_pad(jnp.concatenate([f[..., :w] for f, w in zip(fields, ZRIM)], axis=-1)), quad),
        rows_of(lane_pad(jnp.concatenate([f[..., cz - w :] for f, w in zip(fields, ZRIM)], axis=-1)), quad),
        "grp",
        False,
    )
    shapes = [(cx, ey, 128), (2, ky, 32, 128)]
    low, high = cut_rows(got[0], shapes), cut_rows(got[1], shapes)
    ends = lane_pad(jnp.concatenate([high[0][..., :ZSIDE], low[0][..., :ZSIDE]], axis=-1))

    def quad_apart(q):
        return jnp.stack([q[..., 32 * i : 32 * i + 32] for i in range(4)], axis=1).reshape(cx, ky, 32, 32)

    after, ahead = quad_apart(high[1]), quad_apart(low[1])

    def k_three(cut):
        return lane_pad(jnp.concatenate([block[cut], after[cut], ahead[cut]], axis=-1))

    got = exchange(
        rows_of(*fields, ends, k_three(slice(0, ERIM))),
        rows_of(*fields, ends, k_three(slice(cx - ERIM, cx))),
        GX,
        True,
    )
    planes = (len(fields) + 1) * cx * ey
    low, high = (cut_rows(g[planes:], [(ERIM, ky, 32, 128)])[0] for g in got)
    below, above = (g.reshape(-1, ey, 128) for g in got)
    k_own = jnp.concatenate([low[..., :32], block, high[..., :32]], axis=0)
    k_ends = jnp.concatenate(
        [
            jnp.concatenate([low[..., 32:64], after, high[..., 32:64]], axis=0),
            jnp.concatenate([low[..., 64:96], ahead, high[..., 64:96]], axis=0),
        ],
        axis=2,
    )

    plane = total_y * total_z
    well_x = (well_cells // plane - start_x + RIM) % total_x
    well_y = well_cells // total_z % total_y - start_y + RIM
    well_z = well_cells % total_z - start_z
    near = (well_z >= -ZRIM[0]) & (well_z < cz + ZRIM[0])
    lane = jnp.where(near, well_z % 256, -1)
    at_x = (jnp.arange(ex, dtype=jnp.int32)[:, None] == well_x[None, :]).astype(F32)
    at_y = (jnp.arange(ey, dtype=jnp.int32)[:, None] == well_y[None, :]).astype(F32)
    at_xy = (at_x[:, None, :] * at_y[None, :, :]).reshape(ex * ey, -1)
    at_z = jnp.where(lane[:, None] == jnp.arange(256, dtype=jnp.int32)[None, :], well_rates[:, None], 0.0)
    source = jnp.dot(at_xy, at_z, precision=lax.Precision.HIGHEST).reshape(ex, ey, 256)
    cells = pltpu.VMEM((ex, ey, 256), F32)
    tall = pltpu.VMEM((cx, cy, 256), F32)
    n = cx + 2 * ERIM
    node = pltpu.VMEM((n - 1, n - 1, 8, 256), F32)
    buf = pltpu.VMEM((ex, ey, 256), F32)
    bp_buf = pltpu.VMEM((n, ey, 256), F32)
    elastic_bufs = [
        pltpu.VMEM((n + 1, n + 1, 8, 256), F32),
        pltpu.VMEM((n - 1, n - 1, 8, 256), F32),
        pltpu.VMEM((n, n - 1, 8, 256), F32),
        pltpu.VMEM((n, n - 1, 8, 256), F32),
    ]
    z_pieces = [(max(i - 1, 0), w, sum(ZRIM[:i]), ZSIDE + sum(ZRIM[:i])) for i, w in enumerate(ZRIM)]
    signs = jnp.asarray(np.broadcast_to(sign.reshape(4, 8, 1), (4, 8, 256)), F32)
    z_range = jnp.stack([start_z, jnp.int32(total_z)]).astype(jnp.int32)
    p1, s1, d_pack, *static = pl.pallas_call(
        first_flow,
        out_shape=[tall, tall, pltpu.VMEM((cx + 1, cy + 1, 8, 128), F32)] + [cells] * 9 + [node] * 2,
        in_specs=[pl.BlockSpec(memory_space=pltpu.SMEM)] * 2 + vmem(15),
        out_specs=vmem(14),
        scratch_shapes=[buf] * 5 + [bp_buf] + elastic_bufs,
        compiler_params=pltpu.CompilerParams(vmem_limit_bytes=26 << 20),
        name="first_iteration",
    )(
        rock_table, z_range, below, above, *fields, ends, end_places(z_pieces),
        pressure_start, conductance, source, k_own, k_ends, signs,
    )

    def ends_of(a):
        return jnp.concatenate([a[..., 128 : 128 + ZR1], a[..., 256 - ZR1 :]], axis=-1)

    parts = [*halves(p1), s1.astype(BF)]
    moving = [a[..., :128] for a in parts] + [lane_pad(jnp.concatenate([ends_of(a) for a in parts], axis=-1))]
    d_bf = d_pack.astype(BF)
    got = exchange(
        rows_of(*moving, d_bf[:, 1 : 1 + ERIM]),
        rows_of(*moving, d_bf[:, cy - ERIM : cy]),
        "gy",
        False,
    )
    shapes = [(cx, cy, 128)] * 4 + [(cx + 1, ERIM, 8, 128)]
    low, high = cut_rows(got[0], shapes), cut_rows(got[1], shapes)
    moving = [jnp.concatenate([low[i], moving[i], high[i]], axis=1) for i in range(4)]
    d_bf = jnp.concatenate([low[4], d_bf, high[4]], axis=1)
    got = exchange(
        rows_of(*moving, d_bf[1 : 1 + ERIM]),
        rows_of(*moving, d_bf[cx - ERIM : cx]),
        GX,
        True,
    )
    planes = len(moving) * cx * ey
    low, high = (cut_rows(g[planes:], [(ERIM, cy + 1 + 2 * ERIM, 8, 128)])[0] for g in got)
    below, above = (g.reshape(-1, ey, 128) for g in got)
    d_bf = jnp.concatenate([low, d_bf, high], axis=0)
    pieces = [(max(i - 1, 0), ZR1, 2 * i * ZR1, (2 * i + 1) * ZR1) for i in range(3)]

    short = jax.ShapeDtypeStruct((cx, cy, cz), F32)
    return pl.pallas_call(
        second_flow,
        out_shape=[short, short],
        in_specs=vmem(14 + 11),
        out_specs=vmem(2),
        scratch_shapes=[buf] * 4 + [bp_buf] + elastic_bufs,
        compiler_params=pltpu.CompilerParams(vmem_limit_bytes=26 << 20),
        name="second_iteration",
    )(
        below, above, *moving, end_places(pieces), p1, s1,
        d_bf, d_pack, k_own, k_ends, signs, *static,
    )


def solution(mesh):
    torus = Mesh(
        mesh.devices.reshape(mesh.shape["grp"], 4, 2, 2, mesh.shape["gy"]),
        ("grp", "gx_0", "gx_1", "gx_2", "gy"),
    )
    return jax.shard_map(
        per_device,
        mesh=torus,
        in_specs=(
            P(GX, "gy", "grp"),
            P(GX, "gy", "grp"),
            P(GX, "gy", "grp"),
            P(GX, "gy", "grp"),
            P(),
            P(),
            P(),
            P(GX, "gy", "grp", None, None),
            P(GX, "gy", "grp", None, None, None, None),
            P(GX, "gy", "grp"),
        ),
        out_specs=(P(GX, "gy", "grp"), P(GX, "gy", "grp")),
        check_vma=False,
    )
```

```python
import jax
import jax.numpy as jnp
import numpy as np
from jax import lax
from jax.experimental import pallas as pl
from jax.experimental.pallas import tpu as pltpu
from jax.sharding import Mesh
from jax.sharding import PartitionSpec as P

ITERS = 2
FLOW_PASSES = 4
MECH_PASSES = 3
OMEGA = 0.6
GX = ("gx_0", "gx_1", "gx_2")
BF = jnp.bfloat16
F32 = jnp.float32
RIM = 8
ZRIM = (13, 13, 13, 13, 10)
ZSIDE = sum(ZRIM)
ZR1 = 7
ERIM = 3


def row_order():
    order = np.zeros((32, 24), np.float32)
    sign = np.zeros((2, 2, 8), np.float32)
    for c in range(3):
        for dx in (0, 1):
            for dy in (0, 1):
                for dz in (0, 1):
                    order[8 * (2 * dx + dy) + 4 * dz + c, 8 * c + 4 * dx + 2 * dy + dz] = 1.0
                    sign[dx, dy, 4 * dz + c] = 0.25 * (2 * (dx, dy, dz)[c] - 1)
    return order, sign


def exchange(to_low, to_high, axis, periodic):
    count = lax.axis_size(axis)
    last = count if periodic else count - 1
    up = [(i, (i + 1) % count) for i in range(last)]
    down = [((i + 1) % count, i) for i in range(last)]
    return lax.ppermute(to_high, axis, up), lax.ppermute(to_low, axis, down)


def rows_of(*parts):
    return jnp.concatenate([p.reshape(-1, 128) for p in parts], axis=0)


def cut_rows(buffer, shapes):
    out, at = [], 0
    for shape in shapes:
        rows = int(np.prod(shape)) // 128
        out.append(buffer[at : at + rows].reshape(shape))
        at += rows
    return out


def lane_pad(a):
    return jnp.pad(a, [(0, 0)] * (a.ndim - 1) + [(0, 128 - a.shape[-1])])


def cut_along(array, dim, peers):
    lengths = array.shape
    parts = array.reshape(*lengths[:dim], peers, lengths[dim] // peers, *lengths[dim + 1 :])
    return jnp.moveaxis(parts, dim, 0)


def joined_along(parts, dim):
    lengths = list(parts.shape[1:])
    lengths[dim] *= parts.shape[0]
    return jnp.moveaxis(parts, 0, dim).reshape(lengths)


def exchange_in_order(parts, axes, order):
    lengths = [lax.axis_size(a) for a in axes]
    parts = parts.reshape(*lengths, *parts.shape[1:])
    for k in order:
        parts = lax.all_to_all(parts, axes[k], split_axis=k, concat_axis=k, tiled=True)
    return parts.reshape(-1, *parts.shape[len(axes) :])


def core_and_chips(array, groups, order, split_dim, concat_dim):
    peers = lax.axis_size(groups[0]) * lax.axis_size(groups[1])
    parts = cut_along(array, split_dim, peers)
    return joined_along(exchange_in_order(parts, groups, order), concat_dim)


def pick(rock, table):
    one_hot = (rock[None] == jnp.arange(table.shape[1], dtype=jnp.int32)[:, None, None, None]).astype(F32)
    return jnp.tensordot(table, one_hot, 1, precision=lax.Precision.HIGHEST)


def transmit(a, b):
    total = a + b
    return 2.0 * a * b / jnp.where(total > 0, total, 1.0)


def roll_up(a, axis):
    return pltpu.roll(a, a.shape[axis] - 1, axis)


def roll_down(a, axis):
    return pltpu.roll(a, 1, axis)


def flow_passes(start, spare, num, tx, ty, tz, inv_den, biot, load, out):
    ex = start.shape[0]
    cx, cy, width = out.shape
    for k in range(1, FLOW_PASSES + 1):
        src = start if k % 2 == 1 else spare
        dst = spare if k % 2 == 1 else start
        lo, hi = 1 + k, ex - 1 - k

        def step(x, carry):
            mid = src[x]
            total = (
                (num[x] + tx[x - 1] * src[x - 1])
                + (tx[x] * src[x + 1] + ty[x] * roll_up(mid, 0))
                + (roll_down(ty[x] * mid, 0) + tz[x] * roll_up(mid, 1))
                + roll_down(tz[x] * mid, 1)
            ) * inv_den[x]
            dst[x] = total
            if k == FLOW_PASSES:
                load[x - lo] = total * biot[x]
            return carry

        lax.fori_loop(lo, hi, step, 0, unroll=2)
    out[...] = start[RIM : RIM + cx, RIM : RIM + cy, :width]


def tile_row():
    return lax.broadcasted_iota(jnp.int32, (8, 256), 0)


def fold(g):
    swapped = pltpu.roll(g, 4, 0)
    return g + jnp.where(tile_row() < 4, roll_down(swapped, 1), roll_up(swapped, 1))


def brick_product(ko, ke, u_own, u_end):
    f_own = jnp.dot(ko, u_own, preferred_element_type=F32)
    f_end = jnp.dot(ke, u_end, preferred_element_type=F32)
    lane = lax.broadcasted_iota(jnp.int32, (32, 128), 1)
    f_end = jnp.where(lane < 64, f_end[:32], f_end[32:])
    return [jnp.concatenate([f_own[8 * q : 8 * q + 8], f_end[8 * q : 8 * q + 8]], axis=1) for q in range(4)]


def spread_rows(products, n, x, low_x, high_x):
    last = None
    for y in range(n):
        now = products(y)
        if last is not None:
            low_x[x, y - 1] = now[0] + last[1]
            high_x[x, y - 1] = now[2] + last[3]
        last = now


def elastic_static(held, k_own, k_ends, step, low_x, high_x):
    n = k_own.shape[0]
    eye = (lax.broadcasted_iota(jnp.int32, (64, 32), 0) % 32) == lax.broadcasted_iota(jnp.int32, (64, 32), 1)
    eye = jnp.where(eye, 1.0, 0.0)
    ones = jnp.ones((32, 128), BF)

    def bricks(x, carry):
        def product(y):
            ko = (k_own[x, y].astype(F32) * eye[:32]).astype(BF)
            ke = (k_ends[x, y].astype(F32) * eye).astype(BF)
            return brick_product(ko, ke, ones, ones)

        spread_rows(product, n, x, low_x, high_x)
        return carry

    lax.fori_loop(0, n, bricks, 0)

    def nodes(i, carry):
        m = RIM - ERIM
        for j in range(n - 1):
            diag = fold(low_x[i + 1, j] + high_x[i, j])
            near = [
                jnp.broadcast_to(held[i + m + a, j + m + b : j + m + b + 1, :], (8, 256))
                for a in (0, 1)
                for b in (0, 1)
            ]
            near = (near[0] + near[1]) + (near[2] + near[3])
            near = near + jnp.where(tile_row() < 4, roll_down(near, 1), roll_up(near, 1))
            loose = jnp.where(near > 0, 0.0, 1.0)
            step[i, j] = jnp.where(diag > 0, OMEGA * loose / jnp.where(diag > 0, diag, 1.0), 0.0)
        return carry

    lax.fori_loop(0, n - 1, nodes, 0)


def elastic_load(bp, signs, load):
    n = bp.shape[0]
    m = RIM - ERIM

    def nodes(i, carry):
        sign = [signs[q] for q in range(4)]
        for j in range(n - 1):
            total = None
            for dx in (0, 1):
                for dy in (0, 1):
                    y = j + m + 1 - dy
                    term = jnp.broadcast_to(bp[i + 1 - dx, y : y + 1, :], (8, 256)) * sign[2 * dx + dy]
                    total = term if total is None else total + term
            load[i, j] = fold(total)
        return carry

    lax.fori_loop(0, n - 1, nodes, 0)


def elastic_pass(rim, disp, load, step, k_own, k_ends, low_x, high_x, cx):
    n, m = cx + 2 * rim, ERIM - rim

    def bricks(x, carry):
        def product(y):
            u = jnp.concatenate([disp[x + m + dx, y + m + dy] for dx in (0, 1) for dy in (0, 1)], axis=0).astype(BF)
            return brick_product(k_own[x + m, y + m], k_ends[x + m, y + m], u[:, :128], u[:, 128:])

        spread_rows(product, n, x, low_x, high_x)
        return carry

    lax.fori_loop(0, n, bricks, 0)

    def nodes(i, carry):
        for j in range(n - 1):
            residual = load[i + m, j + m] - fold(low_x[i + 1, j] + high_x[i, j])
            at = (i + m + 1, j + m + 1)
            rate = step[i + m, j + m]
            disp[at] = jnp.where(rate > 0, disp[at] + rate * residual, 0.0)
        return carry

    lax.fori_loop(0, n - 1, nodes, 0)


def elastic_strain(disp, signs, out):
    cx, cy, width = out.shape

    def cells(x, carry):
        sign = [signs[q] for q in range(4)]
        for y in range(cy):
            total = None
            for dx in (0, 1):
                for dy in (0, 1):
                    term = disp[x + ERIM + dx, y + ERIM + dy] * sign[2 * dx + dy]
                    total = term if total is None else total + term
            out[x, y : y + 1, :] = jnp.sum(total, axis=0, keepdims=True)[:, :width]
        return carry

    lax.fori_loop(0, cx, cells, 0)


def first_flow(
    table, z_range, below, above, f0, f1, f2, f3, f4, ends, place, p_own, c_own, source, k_own, k_ends, signs,
    out, strain, packed, h0, h1, h2, h3, h4, h5, h6, h7,
    base, stress, biot, tx, ty, tz, inv_den, step, sems,
    start, spare, cond, num, held, bp, disp, load, low_x, high_x,
):
    ex, ey = start.shape[0], start.shape[1]
    cx = p_own.shape[0]
    lane = lax.broadcasted_iota(jnp.int32, (ey, 256), 1)
    z_at = jnp.where(lane < 192, lane, lane - 256) + z_range[0]
    z_in = (z_at >= 0) & (z_at < z_range[1])

    def choose(rock, row):
        value = jnp.full(rock.shape, table[row, 3], F32)
        for r in range(3):
            value = jnp.where(rock == float(r), table[row, r], value)
        return value

    def gather(plane, offset):
        def one(i, carry):
            x = i + offset
            apart = jnp.dot(plane(5, i), place[...], preferred_element_type=F32)
            fine = plane(0, i).astype(F32) + plane(1, i).astype(F32)
            start[x] = jnp.concatenate([fine, apart[:, :128]], axis=1)
            cond[x] = jnp.concatenate([plane(2, i).astype(F32), apart[:, 128:256]], axis=1)
            rock = jnp.concatenate([plane(3, i).astype(F32), apart[:, 256:384]], axis=1)
            held[x] = jnp.concatenate([plane(4, i).astype(F32), apart[:, 384:]], axis=1)
            storage = choose(rock, 2)
            strained = choose(rock, 3)
            base[x] = storage
            stress[x] = strained
            biot[x] = jnp.where(z_in, choose(rock, 4), 0.0)
            inv_den[x] = storage + strained
            return carry

        lax.fori_loop(0, RIM, one, 0, unroll=2)

    own = (f0, f1, f2, f3, f4, ends)
    gather(lambda f, i: below[f * RIM + i], 0)
    gather(lambda f, i: own[f][i], RIM)
    gather(lambda f, i: above[f * RIM + i], RIM + cx)
    start[RIM : RIM + cx, RIM : RIM + p_own.shape[1], 0:128] = p_own[...]
    cond[RIM : RIM + cx, RIM : RIM + p_own.shape[1], 0:128] = c_own[...]

    def static_terms(x, carry):
        c = cond[x]
        tx[x] = transmit(c, cond[jnp.minimum(x + 1, ex - 1)])
        t = transmit(c, roll_up(c, 0))
        low = roll_down(t, 0)
        ty[x] = t
        den = inv_den[x] + t + low
        t = transmit(c, roll_up(c, 1))
        low = roll_down(t, 1)
        tz[x] = t
        p = start[x]
        b = base[x] * p + source[x]
        base[x] = b
        num[x] = b + stress[x] * p
        inv_den[x] = 1.0 / (den + t + low + tx[x] + tx[jnp.maximum(x - 1, 0)])
        return carry

    lax.fori_loop(0, ex, static_terms, 0, unroll=2)
    kept = zip((base, stress, biot, tx, ty, tz, inv_den, step), (h0, h1, h2, h3, h4, h5, h6, h7))
    saves = [pltpu.make_async_copy(a, h, sems.at[i]) for i, (a, h) in enumerate(kept)]
    for save in saves[:7]:
        save.start()
    flow_passes(start, spare, num, tx, ty, tz, inv_den, biot, bp, out)
    elastic_static(held, k_own, k_ends, step, low_x, high_x)
    saves[7].start()
    elastic_load(bp, signs, load)

    def first_pass(i, carry):
        for j in range(step.shape[1]):
            disp[i + 1, j + 1] = step[i, j] * load[i, j]
        return carry

    lax.fori_loop(0, step.shape[0], first_pass, 0)
    for k in range(1, MECH_PASSES):
        elastic_pass(ERIM - k, disp, load, step, k_own, k_ends, low_x, high_x, cx)
    elastic_strain(disp, signs, strain)

    def pack(i, carry):
        for j in range(packed.shape[1]):
            d = disp[i + ERIM, j + ERIM]
            packed[i, j] = jnp.where(tile_row()[:, :128] < 4, d[:, :128], pltpu.roll(d[:, 128:], 4, 0))
        return carry

    lax.fori_loop(0, packed.shape[0], pack, 0)
    for save in saves:
        save.wait()


def second_flow(
    below, above, f0, f1, f2, ends, place, p_own, s_own, d_ext, d_own, k_own, k_ends, signs,
    h0, h1, h2, h3, h4, h5, h6, h7,
    out, strain_out, base, stress, biot, tx, ty, tz, inv_den, step, sems,
    start, spare, num, strain, bp, disp, load, low_x, high_x,
):
    ex = start.shape[0]
    cx, cy = p_own.shape[0], p_own.shape[1]

    kept = zip((h0, h1, h2, h3, h4, h5, h6, h7), (base, stress, biot, tx, ty, tz, inv_den, step))
    loads = [pltpu.make_async_copy(h, a, sems.at[i]) for i, (h, a) in enumerate(kept)]
    for one_load in loads:
        one_load.start()

    def gather(plane, offset):
        def one(i, carry):
            x = i + offset
            apart = jnp.dot(plane(3, i), place[...], preferred_element_type=F32)
            fine = plane(0, i).astype(F32) + plane(1, i).astype(F32)
            start[x] = jnp.concatenate([fine, apart[:, :128]], axis=1)
            strain[x] = jnp.concatenate([plane(2, i).astype(F32), apart[:, 128:]], axis=1)
            return carry

        lax.fori_loop(0, RIM, one, 0, unroll=2)

    own = (f0, f1, f2, ends)
    gather(lambda f, i: below[f * RIM + i], 0)
    gather(lambda f, i: own[f][i], RIM)
    gather(lambda f, i: above[f * RIM + i], RIM + cx)
    start[RIM : RIM + cx, RIM : RIM + cy, :] = p_own[...]
    strain[RIM : RIM + cx, RIM : RIM + cy, :] = s_own[...]

    for one_load in loads[:7]:
        one_load.wait()

    def numerator(x, carry):
        num[x] = base[x] + stress[x] * start[x] - biot[x] * strain[x]
        return carry

    lax.fori_loop(2, ex - 2, numerator, 0, unroll=2)
    flow_passes(start, spare, num, tx, ty, tz, inv_den, biot, bp, out)
    elastic_load(bp, signs, load)

    loads[7].wait()

    def unpacked(d):
        wide = jnp.concatenate([d, pltpu.roll(d, 4, 0)], axis=1)
        return jnp.where(tile_row() < 4, wide, pltpu.roll(roll_up(wide, 1), 4, 0))

    def unpack(i, carry):
        for j in range(d_ext.shape[1]):
            disp[i, j] = unpacked(d_ext[i, j].astype(F32))
        return carry

    lax.fori_loop(0, d_ext.shape[0], unpack, 0)

    def unpack_own(i, carry):
        for j in range(d_own.shape[1]):
            disp[i + ERIM, j + ERIM] = unpacked(d_own[i, j])
        return carry

    lax.fori_loop(0, d_own.shape[0], unpack_own, 0)
    for k in range(MECH_PASSES):
        elastic_pass(ERIM - k, disp, load, step, k_own, k_ends, low_x, high_x, cx)
    elastic_strain(disp, signs, strain_out)


def pack_blocks(held, lanes_of, out):
    def one(g, carry):
        parts = [jnp.dot(held[4 * g + j], lanes_of[j], preferred_element_type=F32) for j in range(4)]
        out[g] = ((parts[0] + parts[1]) + (parts[2] + parts[3])).astype(BF)
        return carry

    lax.fori_loop(0, out.shape[0], one, 0, unroll=4)


def vmem(n):
    return [pl.BlockSpec(memory_space=pltpu.VMEM)] * n


def end_places(pieces):
    place = np.zeros((128, 128 * (1 + max(p[0] for p in pieces))), np.float32)
    for tile, width, after, ahead in pieces:
        for t in range(width):
            place[after + t, 128 * tile + t] = 1.0
            place[ahead + t, 128 * tile + 128 - width + t] = 1.0
    return jnp.asarray(place, BF)


def halves(a):
    high = lax.reduce_precision(a, 8, 7)
    return high.astype(BF), (a - high).astype(BF)


def per_device(
    pressure_start,
    saturation,
    permeability,
    rock_type,
    rock_table,
    well_cells,
    well_rates,
    owner_map,
    stiffness,
    anchored,
):
    cx, cy, cz = pressure_start.shape
    count_x = lax.axis_size(GX)
    total_x = cx * count_x
    total_y = cy * lax.axis_size("gy")
    total_z = cz * lax.axis_size("grp")
    start_x = lax.axis_index(GX) * cx
    start_y = lax.axis_index("gy") * cy
    start_z = lax.axis_index("grp") * cz
    order, sign = row_order()
    ex, ey = cx + 2 * RIM, cy + 2 * RIM

    owners = owner_map.reshape(-1)
    capacity = stiffness.shape[4]
    one_hot = (owners[:, None] == jnp.arange(count_x, dtype=jnp.int32)[None, :]).astype(jnp.int32)
    before = jnp.cumsum(one_hot, axis=0) - one_hot
    brick_rank = jnp.sum(before * one_hot, axis=1)
    lanes_of = np.zeros((4, 24, 128), np.float32)
    for j in range(4):
        lanes_of[j, :, 32 * j : 32 * j + 32] = order.T
    lanes_of = jnp.asarray(lanes_of, BF)
    packed = pl.pallas_call(
        pack_blocks,
        out_shape=jax.ShapeDtypeStruct((count_x * (capacity // 4), 24, 128), BF),
        in_specs=vmem(2),
        out_specs=vmem(1)[0],
        compiler_params=pltpu.CompilerParams(vmem_limit_bytes=26 << 20),
        name="pack_blocks",
    )(stiffness.reshape(count_x * capacity, 24, 24), lanes_of)
    packed = packed.reshape(count_x, capacity // 4, 24, 128)
    fetched = core_and_chips(packed, (("gx_0", "gx_1"), "gx_2"), (1, 0), 0, 0)
    groups = fetched.reshape(count_x * (capacity // 4), 24, 128)[owners * (capacity // 4) + brick_rank // 4]
    lane_at = lax.broadcasted_iota(jnp.int32, groups.shape, 2) // 32
    groups = jnp.where(lane_at == (brick_rank % 4)[:, None, None], groups, 0)
    fold = jnp.asarray(np.tile(np.eye(32, dtype=np.float32), (4, 1)), BF)
    half = jnp.einsum("brm,mc->brc", groups, fold, preferred_element_type=F32).astype(BF)
    block = jnp.einsum("ar,brc->bac", jnp.asarray(order, BF), half, preferred_element_type=F32).astype(BF)
    block = block.reshape(cx, cy, 32, 32)

    exponents = pick(rock_type, rock_table[:2])
    mobility = jnp.exp(exponents[0] * jnp.log(saturation)) + 2.0 * jnp.exp(
        exponents[1] * jnp.log(1.0 - saturation)
    )
    conductance = permeability * mobility
    fields = [*halves(pressure_start)] + [a.astype(BF) for a in (conductance, rock_type, anchored)]

    def k_lanes(b):
        return lane_pad(jnp.concatenate([b[:, i] for i in range(ERIM)], axis=-1))

    got = exchange(
        rows_of(*fields, k_lanes(block[:, :ERIM])),
        rows_of(*fields, k_lanes(block[:, cy - ERIM :])),
        "gy",
        False,
    )
    shapes = [(cx, cy, cz)] * 5 + [(cx, 32, 128)]
    low, high = cut_rows(got[0], shapes), cut_rows(got[1], shapes)
    fields = [jnp.concatenate([low[i], fields[i], high[i]], axis=1) for i in range(5)]

    def k_apart(lanes):
        return jnp.stack([lanes[:, :, 32 * i : 32 * i + 32] for i in range(ERIM)], axis=1)

    block = jnp.concatenate([k_apart(low[5]), block, k_apart(high[5])], axis=1)
    ky = cy + 2 * ERIM

    quad = block.reshape(2, 4, ky, 32, 32)
    quad = jnp.concatenate([quad[:, i] for i in range(4)], axis=-1)
    got = exchange(
        rows_of(lane_pad(jnp.concatenate([f[..., :w] for f, w in zip(fields, ZRIM)], axis=-1)), quad),
        rows_of(lane_pad(jnp.concatenate([f[..., cz - w :] for f, w in zip(fields, ZRIM)], axis=-1)), quad),
        "grp",
        False,
    )
    shapes = [(cx, ey, 128), (2, ky, 32, 128)]
    low, high = cut_rows(got[0], shapes), cut_rows(got[1], shapes)
    ends = lane_pad(jnp.concatenate([high[0][..., :ZSIDE], low[0][..., :ZSIDE]], axis=-1))

    def quad_apart(q):
        return jnp.stack([q[..., 32 * i : 32 * i + 32] for i in range(4)], axis=1).reshape(cx, ky, 32, 32)

    after, ahead = quad_apart(high[1]), quad_apart(low[1])

    def k_three(cut):
        return lane_pad(jnp.concatenate([block[cut], after[cut], ahead[cut]], axis=-1))

    got = exchange(
        rows_of(*fields, ends, k_three(slice(0, ERIM))),
        rows_of(*fields, ends, k_three(slice(cx - ERIM, cx))),
        GX,
        True,
    )
    planes = (len(fields) + 1) * cx * ey
    low, high = (cut_rows(g[planes:], [(ERIM, ky, 32, 128)])[0] for g in got)
    below, above = (g.reshape(-1, ey, 128) for g in got)
    k_own = jnp.concatenate([low[..., :32], block, high[..., :32]], axis=0)
    k_ends = jnp.concatenate(
        [
            jnp.concatenate([low[..., 32:64], after, high[..., 32:64]], axis=0),
            jnp.concatenate([low[..., 64:96], ahead, high[..., 64:96]], axis=0),
        ],
        axis=2,
    )

    plane = total_y * total_z
    well_x = (well_cells // plane - start_x + RIM) % total_x
    well_y = well_cells // total_z % total_y - start_y + RIM
    well_z = well_cells % total_z - start_z
    near = (well_z >= -ZRIM[0]) & (well_z < cz + ZRIM[0])
    lane = jnp.where(near, well_z % 256, -1)
    at_x = (jnp.arange(ex, dtype=jnp.int32)[:, None] == well_x[None, :]).astype(F32)
    at_y = (jnp.arange(ey, dtype=jnp.int32)[:, None] == well_y[None, :]).astype(F32)
    at_xy = (at_x[:, None, :] * at_y[None, :, :]).reshape(ex * ey, -1)
    at_z = jnp.where(lane[:, None] == jnp.arange(256, dtype=jnp.int32)[None, :], well_rates[:, None], 0.0)
    source = jnp.dot(at_xy, at_z, precision=lax.Precision.HIGHEST).reshape(ex, ey, 256)
    cells = pltpu.HBM((ex, ey, 256), F32)
    tall = pltpu.VMEM((cx, cy, 256), F32)
    n = cx + 2 * ERIM
    node = pltpu.HBM((n - 1, n - 1, 8, 256), F32)
    buf = pltpu.VMEM((ex, ey, 256), F32)
    bp_buf = pltpu.VMEM((n, ey, 256), F32)
    hbm = pl.BlockSpec(memory_space=pltpu.HBM)
    static_bufs = [buf] * 7 + [pltpu.VMEM((n - 1, n - 1, 8, 256), F32), pltpu.SemaphoreType.DMA((8,))]
    elastic_bufs = [
        pltpu.VMEM((n + 1, n + 1, 8, 256), F32),
        pltpu.VMEM((n - 1, n - 1, 8, 256), F32),
        pltpu.VMEM((n, n - 1, 8, 256), F32),
        pltpu.VMEM((n, n - 1, 8, 256), F32),
    ]
    z_pieces = [(max(i - 1, 0), w, sum(ZRIM[:i]), ZSIDE + sum(ZRIM[:i])) for i, w in enumerate(ZRIM)]
    signs = jnp.asarray(np.broadcast_to(sign.reshape(4, 8, 1), (4, 8, 256)), F32)
    z_range = jnp.stack([start_z, jnp.int32(total_z)]).astype(jnp.int32)
    p1, s1, d_pack, *static = pl.pallas_call(
        first_flow,
        out_shape=[tall, tall, pltpu.VMEM((cx + 1, cy + 1, 8, 128), F32)] + [cells] * 7 + [node],
        in_specs=[pl.BlockSpec(memory_space=pltpu.SMEM)] * 2 + vmem(15),
        out_specs=vmem(3) + [hbm] * 8,
        scratch_shapes=static_bufs + [buf] * 5 + [bp_buf] + elastic_bufs,
        compiler_params=pltpu.CompilerParams(vmem_limit_bytes=34 << 20),
        name="first_iteration",
    )(
        rock_table, z_range, below, above, *fields, ends, end_places(z_pieces),
        pressure_start, conductance, source, k_own, k_ends, signs,
    )

    def ends_of(a):
        return jnp.concatenate([a[..., 128 : 128 + ZR1], a[..., 256 - ZR1 :]], axis=-1)

    parts = [*halves(p1), s1.astype(BF)]
    moving = [a[..., :128] for a in parts] + [lane_pad(jnp.concatenate([ends_of(a) for a in parts], axis=-1))]
    d_bf = d_pack.astype(BF)
    got = exchange(
        rows_of(*moving, d_bf[:, 1 : 1 + ERIM]),
        rows_of(*moving, d_bf[:, cy - ERIM : cy]),
        "gy",
        False,
    )
    shapes = [(cx, cy, 128)] * 4 + [(cx + 1, ERIM, 8, 128)]
    low, high = cut_rows(got[0], shapes), cut_rows(got[1], shapes)
    moving = [jnp.concatenate([low[i], moving[i], high[i]], axis=1) for i in range(4)]
    d_bf = jnp.concatenate([low[4], d_bf, high[4]], axis=1)
    got = exchange(
        rows_of(*moving, d_bf[1 : 1 + ERIM]),
        rows_of(*moving, d_bf[cx - ERIM : cx]),
        GX,
        True,
    )
    planes = len(moving) * cx * ey
    low, high = (cut_rows(g[planes:], [(ERIM, cy + 1 + 2 * ERIM, 8, 128)])[0] for g in got)
    below, above = (g.reshape(-1, ey, 128) for g in got)
    d_bf = jnp.concatenate([low, d_bf, high], axis=0)
    pieces = [(max(i - 1, 0), ZR1, 2 * i * ZR1, (2 * i + 1) * ZR1) for i in range(3)]

    static = [pltpu.with_memory_space_constraint(a, pltpu.HBM) for a in static]
    short = jax.ShapeDtypeStruct((cx, cy, cz), F32)
    return pl.pallas_call(
        second_flow,
        out_shape=[short, short],
        in_specs=vmem(14) + [hbm] * 8,
        out_specs=vmem(2),
        scratch_shapes=static_bufs + [buf] * 4 + [bp_buf] + elastic_bufs,
        compiler_params=pltpu.CompilerParams(vmem_limit_bytes=34 << 20),
        name="second_iteration",
    )(
        below, above, *moving, end_places(pieces), p1, s1,
        d_bf, d_pack, k_own, k_ends, signs, *static,
    )


def solution(mesh):
    torus = Mesh(
        mesh.devices.reshape(mesh.shape["grp"], 4, 2, 2, mesh.shape["gy"]),
        ("grp", "gx_0", "gx_1", "gx_2", "gy"),
    )
    return jax.shard_map(
        per_device,
        mesh=torus,
        in_specs=(
            P(GX, "gy", "grp"),
            P(GX, "gy", "grp"),
            P(GX, "gy", "grp"),
            P(GX, "gy", "grp"),
            P(),
            P(),
            P(),
            P(GX, "gy", "grp", None, None),
            P(GX, "gy", "grp", None, None, None, None),
            P(GX, "gy", "grp"),
        ),
        out_specs=(P(GX, "gy", "grp"), P(GX, "gy", "grp")),
        check_vma=False,
    )
```

```python
import jax
import jax.numpy as jnp
import numpy as np
from jax import lax
from jax.experimental import pallas as pl
from jax.experimental.pallas import tpu as pltpu
from jax.sharding import Mesh
from jax.sharding import PartitionSpec as P

ITERS = 2
FLOW_PASSES = 4
MECH_PASSES = 3
OMEGA = 0.6
GX = ("gx_0", "gx_1", "gx_2")
BF = jnp.bfloat16
F32 = jnp.float32
RIM = 8
ZRIM = (13, 13, 13, 13, 10)
ZSIDE = sum(ZRIM)
ZR1 = 7
ERIM = 3


def row_order():
    order = np.zeros((32, 24), np.float32)
    sign = np.zeros((2, 2, 8), np.float32)
    for c in range(3):
        for dx in (0, 1):
            for dy in (0, 1):
                for dz in (0, 1):
                    order[8 * (2 * dx + dy) + 4 * dz + c, 8 * c + 4 * dx + 2 * dy + dz] = 1.0
                    sign[dx, dy, 4 * dz + c] = 0.25 * (2 * (dx, dy, dz)[c] - 1)
    return order, sign


def exchange(to_low, to_high, axis, periodic):
    count = lax.axis_size(axis)
    last = count if periodic else count - 1
    up = [(i, (i + 1) % count) for i in range(last)]
    down = [((i + 1) % count, i) for i in range(last)]
    return lax.ppermute(to_high, axis, up), lax.ppermute(to_low, axis, down)


def rows_of(*parts):
    return jnp.concatenate([p.reshape(-1, 128) for p in parts], axis=0)


def cut_rows(buffer, shapes):
    out, at = [], 0
    for shape in shapes:
        rows = int(np.prod(shape)) // 128
        out.append(buffer[at : at + rows].reshape(shape))
        at += rows
    return out


def lane_pad(a):
    return jnp.pad(a, [(0, 0)] * (a.ndim - 1) + [(0, 128 - a.shape[-1])])


def cut_along(array, dim, peers):
    lengths = array.shape
    parts = array.reshape(*lengths[:dim], peers, lengths[dim] // peers, *lengths[dim + 1 :])
    return jnp.moveaxis(parts, dim, 0)


def joined_along(parts, dim):
    lengths = list(parts.shape[1:])
    lengths[dim] *= parts.shape[0]
    return jnp.moveaxis(parts, 0, dim).reshape(lengths)


def exchange_in_order(parts, axes, order):
    lengths = [lax.axis_size(a) for a in axes]
    parts = parts.reshape(*lengths, *parts.shape[1:])
    for k in order:
        parts = lax.all_to_all(parts, axes[k], split_axis=k, concat_axis=k, tiled=True)
    return parts.reshape(-1, *parts.shape[len(axes) :])


def core_and_chips(array, groups, order, split_dim, concat_dim):
    peers = lax.axis_size(groups[0]) * lax.axis_size(groups[1])
    parts = cut_along(array, split_dim, peers)
    return joined_along(exchange_in_order(parts, groups, order), concat_dim)


def pick(rock, table):
    one_hot = (rock[None] == jnp.arange(table.shape[1], dtype=jnp.int32)[:, None, None, None]).astype(F32)
    return jnp.tensordot(table, one_hot, 1, precision=lax.Precision.HIGHEST)


def transmit(a, b):
    total = a + b
    return 2.0 * a * b / jnp.where(total > 0, total, 1.0)


def roll_up(a, axis):
    return pltpu.roll(a, a.shape[axis] - 1, axis)


def roll_down(a, axis):
    return pltpu.roll(a, 1, axis)


def flow_passes(start, spare, num, tx, ty, tz, inv_den, biot, load, out):
    ex = start.shape[0]
    cx, cy, width = out.shape
    for k in range(1, FLOW_PASSES + 1):
        src = start if k % 2 == 1 else spare
        dst = spare if k % 2 == 1 else start
        lo, hi = 1 + k, ex - 1 - k

        def step(x, carry):
            mid = src[x]
            total = (
                (num[x] + tx[x - 1] * src[x - 1])
                + (tx[x] * src[x + 1] + ty[x] * roll_up(mid, 0))
                + (roll_down(ty[x] * mid, 0) + tz[x] * roll_up(mid, 1))
                + roll_down(tz[x] * mid, 1)
            ) * inv_den[x]
            dst[x] = total
            if k == FLOW_PASSES:
                load[x - lo] = total * biot[x]
            return carry

        lax.fori_loop(lo, hi, step, 0, unroll=2)
    out[...] = start[RIM : RIM + cx, RIM : RIM + cy, :width]


def tile_row():
    return lax.broadcasted_iota(jnp.int32, (8, 256), 0)


def fold(g):
    swapped = pltpu.roll(g, 4, 0)
    return g + jnp.where(tile_row() < 4, roll_down(swapped, 1), roll_up(swapped, 1))


def brick_product(ko, ke, u_own, u_end):
    f_own = jnp.dot(ko, u_own, preferred_element_type=F32)
    f_end = jnp.dot(ke, u_end, preferred_element_type=F32)
    lane = lax.broadcasted_iota(jnp.int32, (32, 128), 1)
    f_end = jnp.where(lane < 64, f_end[:32], f_end[32:])
    return [jnp.concatenate([f_own[8 * q : 8 * q + 8], f_end[8 * q : 8 * q + 8]], axis=1) for q in range(4)]


def spread_rows(products, n, x, low_x, high_x):
    last = None
    for y in range(n):
        now = products(y)
        if last is not None:
            low_x[x, y - 1] = now[0] + last[1]
            high_x[x, y - 1] = now[2] + last[3]
        last = now


def elastic_static(held, k_own, k_ends, step, low_x, high_x):
    n = k_own.shape[0]
    eye = (lax.broadcasted_iota(jnp.int32, (64, 32), 0) % 32) == lax.broadcasted_iota(jnp.int32, (64, 32), 1)
    eye = jnp.where(eye, 1.0, 0.0)
    ones = jnp.ones((32, 128), BF)

    def bricks(x, carry):
        def product(y):
            ko = (k_own[x, y].astype(F32) * eye[:32]).astype(BF)
            ke = (k_ends[x, y].astype(F32) * eye).astype(BF)
            return brick_product(ko, ke, ones, ones)

        spread_rows(product, n, x, low_x, high_x)
        return carry

    lax.fori_loop(0, n, bricks, 0)

    def nodes(i, carry):
        m = RIM - ERIM
        for j in range(n - 1):
            diag = fold(low_x[i + 1, j] + high_x[i, j])
            near = [
                jnp.broadcast_to(held[i + m + a, j + m + b : j + m + b + 1, :], (8, 256))
                for a in (0, 1)
                for b in (0, 1)
            ]
            near = (near[0] + near[1]) + (near[2] + near[3])
            near = near + jnp.where(tile_row() < 4, roll_down(near, 1), roll_up(near, 1))
            loose = jnp.where(near > 0, 0.0, 1.0)
            step[i, j] = jnp.where(diag > 0, OMEGA * loose / jnp.where(diag > 0, diag, 1.0), 0.0)
        return carry

    lax.fori_loop(0, n - 1, nodes, 0)


def elastic_load(bp, signs, load):
    n = bp.shape[0]
    m = RIM - ERIM

    def nodes(i, carry):
        sign = [signs[q] for q in range(4)]
        for j in range(n - 1):
            total = None
            for dx in (0, 1):
                for dy in (0, 1):
                    y = j + m + 1 - dy
                    term = jnp.broadcast_to(bp[i + 1 - dx, y : y + 1, :], (8, 256)) * sign[2 * dx + dy]
                    total = term if total is None else total + term
            load[i, j] = fold(total)
        return carry

    lax.fori_loop(0, n - 1, nodes, 0)


def elastic_pass(rim, disp, load, step, k_own, k_ends, low_x, high_x, cx):
    n, m = cx + 2 * rim, ERIM - rim

    def bricks(x, carry):
        def product(y):
            u = jnp.concatenate([disp[x + m + dx, y + m + dy] for dx in (0, 1) for dy in (0, 1)], axis=0).astype(BF)
            return brick_product(k_own[x + m, y + m], k_ends[x + m, y + m], u[:, :128], u[:, 128:])

        spread_rows(product, n, x, low_x, high_x)
        return carry

    lax.fori_loop(0, n, bricks, 0)

    def nodes(i, carry):
        for j in range(n - 1):
            residual = load[i + m, j + m] - fold(low_x[i + 1, j] + high_x[i, j])
            at = (i + m + 1, j + m + 1)
            rate = step[i + m, j + m]
            disp[at] = jnp.where(rate > 0, disp[at] + rate * residual, 0.0)
        return carry

    lax.fori_loop(0, n - 1, nodes, 0)


def elastic_strain(disp, signs, out):
    cx, cy, width = out.shape

    def cells(x, carry):
        sign = [signs[q] for q in range(4)]
        for y in range(cy):
            total = None
            for dx in (0, 1):
                for dy in (0, 1):
                    term = disp[x + ERIM + dx, y + ERIM + dy] * sign[2 * dx + dy]
                    total = term if total is None else total + term
            out[x, y : y + 1, :] = jnp.sum(total, axis=0, keepdims=True)[:, :width]
        return carry

    lax.fori_loop(0, cx, cells, 0)


def first_flow(
    table, z_range, below, above, f0, f1, f2, f3, f4, ends, place, p_own, c_own, source, k_own, k_ends, signs,
    out, strain, packed, h0, h1, h2, h3, h4, h5, h6, h7,
    base, stress, biot, tx, ty, tz, inv_den, step, sems,
    start, spare, cond, num, held, bp, disp, load, low_x, high_x,
):
    ex, ey = start.shape[0], start.shape[1]
    cx = p_own.shape[0]
    lane = lax.broadcasted_iota(jnp.int32, (ey, 256), 1)
    z_at = jnp.where(lane < 192, lane, lane - 256) + z_range[0]
    z_in = (z_at >= 0) & (z_at < z_range[1])

    def choose(rock, row):
        value = jnp.full(rock.shape, table[row, 3], F32)
        for r in range(3):
            value = jnp.where(rock == float(r), table[row, r], value)
        return value

    def gather(plane, offset):
        def one(i, carry):
            x = i + offset
            apart = jnp.dot(plane(5, i), place[...], preferred_element_type=F32)
            fine = plane(0, i).astype(F32) + plane(1, i).astype(F32)
            start[x] = jnp.concatenate([fine, apart[:, :128]], axis=1)
            cond[x] = jnp.concatenate([plane(2, i).astype(F32), apart[:, 128:256]], axis=1)
            rock = jnp.concatenate([plane(3, i).astype(F32), apart[:, 256:384]], axis=1)
            held[x] = jnp.concatenate([plane(4, i).astype(F32), apart[:, 384:]], axis=1)
            storage = choose(rock, 2)
            strained = choose(rock, 3)
            base[x] = storage
            stress[x] = strained
            biot[x] = jnp.where(z_in, choose(rock, 4), 0.0)
            inv_den[x] = storage + strained
            return carry

        lax.fori_loop(0, RIM, one, 0, unroll=2)

    own = (f0, f1, f2, f3, f4, ends)
    gather(lambda f, i: below[f * RIM + i], 0)
    gather(lambda f, i: own[f][i], RIM)
    gather(lambda f, i: above[f * RIM + i], RIM + cx)
    start[RIM : RIM + cx, RIM : RIM + p_own.shape[1], 0:128] = p_own[...]
    cond[RIM : RIM + cx, RIM : RIM + p_own.shape[1], 0:128] = c_own[...]

    def static_terms(x, carry):
        c = cond[x]
        tx[x] = transmit(c, cond[jnp.minimum(x + 1, ex - 1)])
        t = transmit(c, roll_up(c, 0))
        low = roll_down(t, 0)
        ty[x] = t
        den = inv_den[x] + t + low
        t = transmit(c, roll_up(c, 1))
        low = roll_down(t, 1)
        tz[x] = t
        p = start[x]
        b = base[x] * p + source[x]
        base[x] = b
        num[x] = b + stress[x] * p
        inv_den[x] = 1.0 / (den + t + low + tx[x] + tx[jnp.maximum(x - 1, 0)])
        return carry

    lax.fori_loop(0, ex, static_terms, 0, unroll=2)
    kept = zip((base, stress, biot, tx, ty, tz, inv_den, step), (h0, h1, h2, h3, h4, h5, h6, h7))
    saves = [pltpu.make_async_copy(a, h, sems.at[i]) for i, (a, h) in enumerate(kept)]
    for save in saves[:7]:
        save.start()
    flow_passes(start, spare, num, tx, ty, tz, inv_den, biot, bp, out)
    elastic_static(held, k_own, k_ends, step, low_x, high_x)
    saves[7].start()
    elastic_load(bp, signs, load)

    def first_pass(i, carry):
        for j in range(step.shape[1]):
            disp[i + 1, j + 1] = step[i, j] * load[i, j]
        return carry

    lax.fori_loop(0, step.shape[0], first_pass, 0)
    for k in range(1, MECH_PASSES):
        elastic_pass(ERIM - k, disp, load, step, k_own, k_ends, low_x, high_x, cx)
    elastic_strain(disp, signs, strain)

    def pack(i, carry):
        for j in range(packed.shape[1]):
            d = disp[i + ERIM, j + ERIM]
            packed[i, j] = jnp.where(tile_row()[:, :128] < 4, d[:, :128], pltpu.roll(d[:, 128:], 4, 0))
        return carry

    lax.fori_loop(0, packed.shape[0], pack, 0)
    for save in saves:
        save.wait()


def second_flow(
    below, above, f0, f1, f2, ends, place, p_own, s_own, d_ext, d_own, k_own, k_ends, signs,
    h0, h1, h2, h3, h4, h5, h6, h7,
    out, strain_out, base, stress, biot, tx, ty, tz, inv_den, step, sems,
    start, spare, num, strain, bp, disp, load, low_x, high_x,
):
    ex = start.shape[0]
    cx, cy = p_own.shape[0], p_own.shape[1]

    kept = zip((h0, h1, h2, h3, h4, h5, h6, h7), (base, stress, biot, tx, ty, tz, inv_den, step))
    loads = [pltpu.make_async_copy(h, a, sems.at[i]) for i, (h, a) in enumerate(kept)]
    for one_load in loads:
        one_load.start()

    def gather(plane, offset):
        def one(i, carry):
            x = i + offset
            apart = jnp.dot(plane(3, i), place[...], preferred_element_type=F32)
            fine = plane(0, i).astype(F32) + plane(1, i).astype(F32)
            start[x] = jnp.concatenate([fine, apart[:, :128]], axis=1)
            strain[x] = jnp.concatenate([plane(2, i).astype(F32), apart[:, 128:]], axis=1)
            return carry

        lax.fori_loop(0, RIM, one, 0, unroll=2)

    own = (f0, f1, f2, ends)
    gather(lambda f, i: below[f * RIM + i], 0)
    gather(lambda f, i: own[f][i], RIM)
    gather(lambda f, i: above[f * RIM + i], RIM + cx)
    start[RIM : RIM + cx, RIM : RIM + cy, :] = p_own[...]
    strain[RIM : RIM + cx, RIM : RIM + cy, :] = s_own[...]

    for one_load in loads[:7]:
        one_load.wait()

    def numerator(x, carry):
        num[x] = base[x] + stress[x] * start[x] - biot[x] * strain[x]
        return carry

    lax.fori_loop(2, ex - 2, numerator, 0, unroll=2)
    flow_passes(start, spare, num, tx, ty, tz, inv_den, biot, bp, out)
    elastic_load(bp, signs, load)

    loads[7].wait()

    def unpacked(d):
        wide = jnp.concatenate([d, pltpu.roll(d, 4, 0)], axis=1)
        return jnp.where(tile_row() < 4, wide, pltpu.roll(roll_up(wide, 1), 4, 0))

    def unpack(i, carry):
        for j in range(d_ext.shape[1]):
            disp[i, j] = unpacked(d_ext[i, j].astype(F32))
        return carry

    lax.fori_loop(0, d_ext.shape[0], unpack, 0)

    def unpack_own(i, carry):
        for j in range(d_own.shape[1]):
            disp[i + ERIM, j + ERIM] = unpacked(d_own[i, j])
        return carry

    lax.fori_loop(0, d_own.shape[0], unpack_own, 0)
    for k in range(MECH_PASSES):
        elastic_pass(ERIM - k, disp, load, step, k_own, k_ends, low_x, high_x, cx)
    elastic_strain(disp, signs, strain_out)


def pack_blocks(held, lanes_of, out):
    def one(g, carry):
        parts = [jnp.dot(held[4 * g + j], lanes_of[j], preferred_element_type=F32) for j in range(4)]
        out[g] = ((parts[0] + parts[1]) + (parts[2] + parts[3])).astype(BF)
        return carry

    lax.fori_loop(0, out.shape[0], one, 0, unroll=4)


def vmem(n):
    return [pl.BlockSpec(memory_space=pltpu.VMEM)] * n


def end_places(pieces):
    place = np.zeros((128, 128 * (1 + max(p[0] for p in pieces))), np.float32)
    for tile, width, after, ahead in pieces:
        for t in range(width):
            place[after + t, 128 * tile + t] = 1.0
            place[ahead + t, 128 * tile + 128 - width + t] = 1.0
    return jnp.asarray(place, BF)


def halves(a):
    high = lax.reduce_precision(a, 8, 7)
    return high.astype(BF), (a - high).astype(BF)


def per_device(
    pressure_start,
    saturation,
    permeability,
    rock_type,
    rock_table,
    well_cells,
    well_rates,
    owner_map,
    stiffness,
    anchored,
):
    cx, cy, cz = pressure_start.shape
    count_x = lax.axis_size(GX)
    total_x = cx * count_x
    total_y = cy * lax.axis_size("gy")
    total_z = cz * lax.axis_size("grp")
    start_x = lax.axis_index(GX) * cx
    start_y = lax.axis_index("gy") * cy
    start_z = lax.axis_index("grp") * cz
    order, sign = row_order()
    ex, ey = cx + 2 * RIM, cy + 2 * RIM

    owners = owner_map.reshape(-1)
    capacity = stiffness.shape[4]
    one_hot = (owners[:, None] == jnp.arange(count_x, dtype=jnp.int32)[None, :]).astype(jnp.int32)
    before = jnp.cumsum(one_hot, axis=0) - one_hot
    brick_rank = jnp.sum(before * one_hot, axis=1)
    lanes_of = np.zeros((4, 24, 128), np.float32)
    for j in range(4):
        lanes_of[j, :, 32 * j : 32 * j + 32] = order.T
    lanes_of = jnp.asarray(lanes_of, BF)
    packed = pl.pallas_call(
        pack_blocks,
        out_shape=jax.ShapeDtypeStruct((count_x * (capacity // 4), 24, 128), BF),
        in_specs=vmem(2),
        out_specs=vmem(1)[0],
        compiler_params=pltpu.CompilerParams(vmem_limit_bytes=26 << 20),
        name="pack_blocks",
    )(stiffness.reshape(count_x * capacity, 24, 24), lanes_of)
    packed = packed.reshape(count_x, capacity // 4, 24, 128)
    fetched = core_and_chips(packed, (("gx_0", "gx_1"), "gx_2"), (1, 0), 0, 0)
    groups = fetched.reshape(count_x * (capacity // 4), 24, 128)[owners * (capacity // 4) + brick_rank // 4]
    lane_at = lax.broadcasted_iota(jnp.int32, groups.shape, 2) // 32
    groups = jnp.where(lane_at == (brick_rank % 4)[:, None, None], groups, 0)
    fold = jnp.asarray(np.tile(np.eye(32, dtype=np.float32), (4, 1)), BF)
    half = jnp.einsum("brm,mc->brc", groups, fold, preferred_element_type=F32).astype(BF)
    block = jnp.einsum("ar,brc->bac", jnp.asarray(order, BF), half, preferred_element_type=F32).astype(BF)
    block = block.reshape(cx, cy, 32, 32)

    exponents = pick(rock_type, rock_table[:2])
    mobility = jnp.exp(exponents[0] * jnp.log(saturation)) + 2.0 * jnp.exp(
        exponents[1] * jnp.log(1.0 - saturation)
    )
    conductance = permeability * mobility
    fields = [*halves(pressure_start)] + [a.astype(BF) for a in (conductance, rock_type, anchored)]

    def k_lanes(b):
        return lane_pad(jnp.concatenate([b[:, i] for i in range(ERIM)], axis=-1))

    got = exchange(
        rows_of(*fields, k_lanes(block[:, :ERIM])),
        rows_of(*fields, k_lanes(block[:, cy - ERIM :])),
        "gy",
        False,
    )
    shapes = [(cx, cy, cz)] * 5 + [(cx, 32, 128)]
    low, high = cut_rows(got[0], shapes), cut_rows(got[1], shapes)
    fields = [jnp.concatenate([low[i], fields[i], high[i]], axis=1) for i in range(5)]

    def k_apart(lanes):
        return jnp.stack([lanes[:, :, 32 * i : 32 * i + 32] for i in range(ERIM)], axis=1)

    block = jnp.concatenate([k_apart(low[5]), block, k_apart(high[5])], axis=1)
    ky = cy + 2 * ERIM

    quad = block.reshape(2, 4, ky, 32, 32)
    quad = jnp.concatenate([quad[:, i] for i in range(4)], axis=-1)
    got = exchange(
        rows_of(lane_pad(jnp.concatenate([f[..., :w] for f, w in zip(fields, ZRIM)], axis=-1)), quad),
        rows_of(lane_pad(jnp.concatenate([f[..., cz - w :] for f, w in zip(fields, ZRIM)], axis=-1)), quad),
        "grp",
        False,
    )
    shapes = [(cx, ey, 128), (2, ky, 32, 128)]
    low, high = cut_rows(got[0], shapes), cut_rows(got[1], shapes)
    ends = lane_pad(jnp.concatenate([high[0][..., :ZSIDE], low[0][..., :ZSIDE]], axis=-1))

    def quad_apart(q):
        return jnp.stack([q[..., 32 * i : 32 * i + 32] for i in range(4)], axis=1).reshape(cx, ky, 32, 32)

    after, ahead = quad_apart(high[1]), quad_apart(low[1])

    def k_three(cut):
        return lane_pad(jnp.concatenate([block[cut], after[cut], ahead[cut]], axis=-1))

    got = exchange(
        rows_of(*fields, ends, k_three(slice(0, ERIM))),
        rows_of(*fields, ends, k_three(slice(cx - ERIM, cx))),
        GX,
        True,
    )
    planes = (len(fields) + 1) * cx * ey
    low, high = (cut_rows(g[planes:], [(ERIM, ky, 32, 128)])[0] for g in got)
    below, above = (g.reshape(-1, ey, 128) for g in got)
    k_own = jnp.concatenate([low[..., :32], block, high[..., :32]], axis=0)
    k_ends = jnp.concatenate(
        [
            jnp.concatenate([low[..., 32:64], after, high[..., 32:64]], axis=0),
            jnp.concatenate([low[..., 64:96], ahead, high[..., 64:96]], axis=0),
        ],
        axis=2,
    )

    plane = total_y * total_z
    well_x = (well_cells // plane - start_x + RIM) % total_x
    well_y = well_cells // total_z % total_y - start_y + RIM
    well_z = well_cells % total_z - start_z
    near = (well_z >= -ZRIM[0]) & (well_z < cz + ZRIM[0])
    lane = jnp.where(near, well_z % 256, -1)
    at_x = (jnp.arange(ex, dtype=jnp.int32)[:, None] == well_x[None, :]).astype(F32)
    at_y = (jnp.arange(ey, dtype=jnp.int32)[:, None] == well_y[None, :]).astype(F32)
    at_xy = (at_x[:, None, :] * at_y[None, :, :]).reshape(ex * ey, -1)
    at_z = jnp.where(lane[:, None] == jnp.arange(256, dtype=jnp.int32)[None, :], well_rates[:, None], 0.0)
    source = jnp.dot(at_xy, at_z, precision=lax.Precision.HIGHEST).reshape(ex, ey, 256)
    cells = pltpu.HBM((ex, ey, 256), F32)
    tall = pltpu.HBM((cx, cy, 256), F32)
    n = cx + 2 * ERIM
    node = pltpu.HBM((n - 1, n - 1, 8, 256), F32)
    buf = pltpu.VMEM((ex, ey, 256), F32)
    bp_buf = pltpu.VMEM((n, ey, 256), F32)
    hbm = pl.BlockSpec(memory_space=pltpu.HBM)
    static_bufs = [buf] * 7 + [pltpu.VMEM((n - 1, n - 1, 8, 256), F32), pltpu.SemaphoreType.DMA((8,))]
    elastic_bufs = [
        pltpu.VMEM((n + 1, n + 1, 8, 256), F32),
        pltpu.VMEM((n - 1, n - 1, 8, 256), F32),
        pltpu.VMEM((n, n - 1, 8, 256), F32),
        pltpu.VMEM((n, n - 1, 8, 256), F32),
    ]
    z_pieces = [(max(i - 1, 0), w, sum(ZRIM[:i]), ZSIDE + sum(ZRIM[:i])) for i, w in enumerate(ZRIM)]
    signs = jnp.asarray(np.broadcast_to(sign.reshape(4, 8, 1), (4, 8, 256)), F32)
    z_range = jnp.stack([start_z, jnp.int32(total_z)]).astype(jnp.int32)
    p1, s1, d_pack, *static = pl.pallas_call(
        first_flow,
        out_shape=[tall, tall, pltpu.HBM((cx + 1, cy + 1, 8, 128), F32)] + [cells] * 7 + [node],
        in_specs=[pl.BlockSpec(memory_space=pltpu.SMEM)] * 2 + vmem(15),
        out_specs=vmem(3) + [hbm] * 8,
        scratch_shapes=static_bufs + [buf] * 5 + [bp_buf] + elastic_bufs,
        compiler_params=pltpu.CompilerParams(vmem_limit_bytes=34 << 20),
        name="first_iteration",
    )(
        rock_table, z_range, below, above, *fields, ends, end_places(z_pieces),
        pressure_start, conductance, source, k_own, k_ends, signs,
    )

    def ends_of(a):
        return jnp.concatenate([a[..., 128 : 128 + ZR1], a[..., 256 - ZR1 :]], axis=-1)

    parts = [*halves(p1), s1.astype(BF)]
    moving = [a[..., :128] for a in parts] + [lane_pad(jnp.concatenate([ends_of(a) for a in parts], axis=-1))]
    d_bf = d_pack.astype(BF)
    got = exchange(
        rows_of(*moving, d_bf[:, 1 : 1 + ERIM]),
        rows_of(*moving, d_bf[:, cy - ERIM : cy]),
        "gy",
        False,
    )
    shapes = [(cx, cy, 128)] * 4 + [(cx + 1, ERIM, 8, 128)]
    low, high = cut_rows(got[0], shapes), cut_rows(got[1], shapes)
    moving = [jnp.concatenate([low[i], moving[i], high[i]], axis=1) for i in range(4)]
    d_bf = jnp.concatenate([low[4], d_bf, high[4]], axis=1)
    got = exchange(
        rows_of(*moving, d_bf[1 : 1 + ERIM]),
        rows_of(*moving, d_bf[cx - ERIM : cx]),
        GX,
        True,
    )
    planes = len(moving) * cx * ey
    low, high = (cut_rows(g[planes:], [(ERIM, cy + 1 + 2 * ERIM, 8, 128)])[0] for g in got)
    below, above = (g.reshape(-1, ey, 128) for g in got)
    d_bf = jnp.concatenate([low, d_bf, high], axis=0)
    pieces = [(max(i - 1, 0), ZR1, 2 * i * ZR1, (2 * i + 1) * ZR1) for i in range(3)]

    static = [pltpu.with_memory_space_constraint(a, pltpu.HBM) for a in static]
    short = jax.ShapeDtypeStruct((cx, cy, cz), F32)
    return pl.pallas_call(
        second_flow,
        out_shape=[short, short],
        in_specs=vmem(14) + [hbm] * 8,
        out_specs=vmem(2),
        scratch_shapes=static_bufs + [buf] * 4 + [bp_buf] + elastic_bufs,
        compiler_params=pltpu.CompilerParams(vmem_limit_bytes=34 << 20),
        name="second_iteration",
    )(
        below, above, *moving, end_places(pieces), p1, s1,
        d_bf, d_pack, k_own, k_ends, signs, *static,
    )


def solution(mesh):
    torus = Mesh(
        mesh.devices.reshape(mesh.shape["grp"], 4, 2, 2, mesh.shape["gy"]),
        ("grp", "gx_0", "gx_1", "gx_2", "gy"),
    )
    return jax.shard_map(
        per_device,
        mesh=torus,
        in_specs=(
            P(GX, "gy", "grp"),
            P(GX, "gy", "grp"),
            P(GX, "gy", "grp"),
            P(GX, "gy", "grp"),
            P(),
            P(),
            P(),
            P(GX, "gy", "grp", None, None),
            P(GX, "gy", "grp", None, None, None, None),
            P(GX, "gy", "grp"),
        ),
        out_specs=(P(GX, "gy", "grp"), P(GX, "gy", "grp")),
        check_vma=False,
    )
```
